8 devices in a mesh: dp: 1 (over z), sp: 8 (over y, x, core).
Axes of the slice: x: 2, y: 2, z: 1, core: 2. Of those that a mesh axis runs over, the one named last changes fastest.
Arguments:
- tokens: bfloat16 [256, 2048], P('dp')
- w_query: bfloat16 [2048, 2048], replicated
- w_key: bfloat16 [2048, 256], replicated
- w_value: bfloat16 [2048, 256], replicated
- w_out: bfloat16 [2048, 2048], P('sp')
- k_cache: bfloat16 [256, 2048, 256], P('dp', 'sp')
- v_cache: bfloat16 [256, 2048, 256], P('dp', 'sp')
- positions: int32 [256], P('dp')
Outputs:
- output 1: bfloat16 [256, 2048], P('dp')
- output 2: bfloat16 [256, 2048, 256], P('dp', 'sp')
- output 3: bfloat16 [256, 2048, 256], P('dp', 'sp')
All inputs are finite; a program needn't handle non-finite values.
Results may differ from the reference program's by a relative error of at most 0.00427737.
Values are sent between devices in bfloat16 or wider.
A program may use at most 1 GiB of HBM per device.

```python
import jax
import jax.numpy as jnp
import math
from jax import lax

BATCH_ROWS = 256
SEQ_LEN = 2048
D_MODEL = 2048
N_HEADS = 8
HEAD_DIM = 256
GAIN_BLOCK = 32


def setup_inputs(seed: int = 0, part: int = 0) -> dict:
    root = jax.random.key(seed)
    shared = jax.random.split(root, 4)
    local = jax.random.split(jax.random.fold_in(root, part), 5)
    q_width = N_HEADS * HEAD_DIM
    align_scale = (math.log(SEQ_LEN) + 0.5) * HEAD_DIM ** -0.5
    tokens = jax.random.normal(local[0], (BATCH_ROWS, D_MODEL), jnp.float32)
    key_raw = jax.random.normal(shared[1], (D_MODEL, HEAD_DIM), jnp.float32)
    w_query = (jax.random.normal(shared[0], (D_MODEL, q_width), jnp.float32) + align_scale * jnp.tile(key_raw, (1, N_HEADS))) * D_MODEL ** -0.5
    w_key = key_raw * D_MODEL ** -0.5
    w_value = jax.random.normal(shared[2], (D_MODEL, HEAD_DIM), jnp.float32) * D_MODEL ** -0.5
    w_out = jax.random.normal(shared[3], (q_width, D_MODEL), jnp.float32) * q_width ** -0.5
    n_blocks = SEQ_LEN // GAIN_BLOCK
    key_gains = jax.random.uniform(local[1], (BATCH_ROWS, n_blocks, 1, 1), jnp.float32, 0.6, 1.6)
    k_cache = (jax.random.normal(local[2], (BATCH_ROWS, n_blocks, GAIN_BLOCK, HEAD_DIM), jnp.float32) * key_gains).reshape(BATCH_ROWS, SEQ_LEN, HEAD_DIM)
    v_cache = jax.random.normal(local[3], (BATCH_ROWS, SEQ_LEN, HEAD_DIM), jnp.float32)
    positions = jax.random.randint(local[4], (BATCH_ROWS,), SEQ_LEN // 4, SEQ_LEN, jnp.int32)
    positions = positions.at[0].set(SEQ_LEN - 1).at[1].set(SEQ_LEN // 4)
    return dict(tokens=tokens.astype(jnp.bfloat16), w_query=w_query.astype(jnp.bfloat16), w_key=w_key.astype(jnp.bfloat16), w_value=w_value.astype(jnp.bfloat16), w_out=w_out.astype(jnp.bfloat16), k_cache=k_cache.astype(jnp.bfloat16), v_cache=v_cache.astype(jnp.bfloat16), positions=positions)


def reference(tokens, w_query, w_key, w_value, w_out, k_cache, v_cache, positions):
    queries = jnp.dot(tokens, w_query, preferred_element_type=jnp.float32).astype(jnp.bfloat16)
    queries = queries.reshape(BATCH_ROWS, N_HEADS, HEAD_DIM)
    key_new = jnp.dot(tokens, w_key, preferred_element_type=jnp.float32).astype(jnp.bfloat16)
    value_new = jnp.dot(tokens, w_value, preferred_element_type=jnp.float32).astype(jnp.bfloat16)
    slot_ids = jnp.arange(SEQ_LEN)
    hit_mask = (slot_ids[None, :] == positions[:, None])[:, :, None]
    k_upd = jnp.where(hit_mask, key_new[:, None, :], k_cache)
    v_upd = jnp.where(hit_mask, value_new[:, None, :], v_cache)

    def one_row(row_args):
        q_row, k_row, v_row, pos_row = row_args
        scores = jnp.dot(q_row, k_row.T, preferred_element_type=jnp.float32) * HEAD_DIM ** -0.5
        scores = jnp.where(slot_ids[None, :] <= pos_row, scores, -jnp.inf)
        weights = jnp.exp(scores - jnp.max(scores, axis=1, keepdims=True))
        weight_sum = jnp.sum(weights, axis=1)
        value_sum = jnp.dot(weights.astype(jnp.bfloat16), v_row, preferred_element_type=jnp.float32)
        return value_sum / weight_sum[:, None]

    head_outs = lax.map(one_row, (queries, k_upd, v_upd, positions))
    attn_heads = head_outs.astype(jnp.bfloat16).reshape(BATCH_ROWS, N_HEADS * HEAD_DIM)
    attn_out = jnp.dot(attn_heads, w_out, preferred_element_type=jnp.float32).astype(jnp.bfloat16)
    return (attn_out, k_upd, v_upd)
```

```python
import functools

import jax
import jax.numpy as jnp
from jax import lax
from jax.experimental import pallas as pl
from jax.experimental.pallas import tpu as pltpu
from jax.sharding import PartitionSpec as P

MESH = pl.DeviceIdType.MESH
F32, BF16 = jnp.float32, jnp.bfloat16
FLOOR = -1e30
HALF = 16
LAG_C, LAG_S, LAG_R = 3, 5, 7


def attend_kernel(dims, pos_ref, q_ref, kn_ref, vn_ref, wo_ref, k_hbm, v_hbm, y_ref, held,
                  part, got_d, mix, got_1, yp, got_2, ybuf, wo2, sem_k, sem_v, sem_w,
                  snd_d, rcv_d, snd_1, rcv_1, snd_2, rcv_2, snd_3, rcv_3, snd_r, rcv_r):
    n_seq, heads, seq_local, hd, groups, slots = dims
    nh, width = HALF, wo_ref.shape[1]
    kb, vb = held.at[0], held.at[1]
    n_blocks, quarter = 2 * groups, width // 4
    body = heads * nh
    scale = hd ** -0.5
    me = lax.axis_index('sp')
    chip, core = me // 2, lax.rem(me, 2)

    def peer(k):
        return {'sp': jnp.bitwise_xor(me, k)}

    def cache_copies(t):
        s = lax.rem(t, slots)
        rows = pl.ds(t * nh, nh)
        return (pltpu.make_async_copy(k_hbm.at[rows], kb.at[s], sem_k.at[s]),
                pltpu.make_async_copy(v_hbm.at[rows], vb.at[s], sem_v.at[s]))

    def load(t):
        for cp in cache_copies(t):
            cp.start()

    for t in range(min(slots, n_blocks)):
        load(t)

    gate = pltpu.get_barrier_semaphore()
    for k in (1, 2, 4, 6):
        pl.semaphore_signal(gate, inc=1, device_id=peer(k), device_id_type=MESH)
    pl.semaphore_wait(gate, 4)

    send_w = pltpu.make_async_remote_copy(wo_ref, wo2.at[core], sem_w.at[0], sem_w.at[1],
                                          device_id=peer(1), device_id_type=MESH)
    send_w.start()
    keep_w = pltpu.make_async_copy(wo_ref, wo2.at[core], sem_w.at[2])

    def d_copy(g):
        return pltpu.make_async_remote_copy(part.at[g, 1 - core], got_d.at[g], snd_d.at[g], rcv_d.at[g],
                                            device_id=peer(1), device_id_type=MESH)

    def one_copy(g, k):
        return pltpu.make_async_remote_copy(mix.at[g, jnp.bitwise_xor(chip, k)], got_1.at[g, k - 1],
                                            snd_1.at[g, k - 1], rcv_1.at[g, k - 1],
                                            device_id=peer(2 * k), device_id_type=MESH)

    def two_copy(g, k):
        return pltpu.make_async_remote_copy(yp.at[g, jnp.bitwise_xor(chip, k)], got_2.at[g, k - 1],
                                            snd_2.at[g, k - 1], rcv_2.at[g, k - 1],
                                            device_id=peer(2 * k), device_id_type=MESH)

    def three_copy(g, k):
        block = ybuf.at[2 * g + core, :, pl.ds(pl.multiple_of(chip * quarter, quarter), quarter)]
        return pltpu.make_async_remote_copy(block, block, snd_3.at[g, k - 1], rcv_3.at[g, k - 1],
                                            device_id=peer(2 * k), device_id_type=MESH)

    def relay_copy(g):
        rows = ybuf.at[2 * g + core]
        return pltpu.make_async_remote_copy(rows, rows, snd_r.at[g], rcv_r.at[g],
                                            device_id=peer(1), device_id_type=MESH)

    slot_ids = lax.broadcasted_iota(jnp.int32, (heads, seq_local), 1)
    lane = lax.broadcasted_iota(jnp.int32, (heads, 128), 1)

    def attend(g, half):
        t = 2 * g + half
        s = lax.rem(t, slots)
        for cp in cache_copies(t):
            cp.wait()
        first = pl.multiple_of(t * nh, nh)
        kn, vn = kn_ref[pl.ds(first, nh), :], vn_ref[pl.ds(first, nh), :]
        scores = []
        for i in range(nh):
            scores.append(lax.dot_general(q_ref[first + i], kb[s, i], (((1,), (1,)), ((), ())),
                                          preferred_element_type=F32) * scale)
        peaks = jnp.full((heads, 128), FLOOR, F32)
        sums = jnp.zeros((heads, 128), F32)
        weights = []
        for i in range(nh):
            p = pos_ref[first + i]
            own = jnp.logical_and(p >= 0, p < seq_local)
            sc = jnp.where(slot_ids < p, scores[i], -jnp.inf)
            fresh = jnp.sum(q_ref[first + i].astype(F32) * kn[i:i + 1, :], axis=1, keepdims=True) * scale
            fresh = jnp.where(own, fresh, -jnp.inf)
            m = jnp.maximum(jnp.maximum(jnp.max(sc, axis=1, keepdims=True), fresh), FLOOR)
            w, wf = jnp.exp(sc - m), jnp.exp(fresh - m)
            peaks = jnp.where(lane == i, m, peaks)
            sums = jnp.where(lane == i, jnp.sum(w, axis=1, keepdims=True) + wf, sums)
            weights.append((w.astype(BF16), wf.astype(BF16).astype(F32)))
        for i in range(nh):
            w, wf = weights[i]
            o = jnp.dot(w, vb[s, i], preferred_element_type=F32) + wf * vn[i:i + 1, :]
            for z in range(2):
                part[g, half, z, pl.ds(i, heads, stride=nh), :] = o[:, z * 128:(z + 1) * 128]
        part[g, half, 0, body:body + heads, :] = peaks
        part[g, half, 1, body:body + heads, :] = sums

        @pl.when(t + slots < n_blocks)
        def _():
            load(t + slots)

    def merge(g):
        d_copy(g).wait_recv()
        a, b = part.at[g, core], got_d.at[g]
        tail = slice(body, body + heads)
        m = jnp.maximum(a[0, tail, :], b[0, tail, :])
        ea, eb = jnp.exp(a[0, tail, :] - m), jnp.exp(b[0, tail, :] - m)
        total = a[1, tail, :] * ea + b[1, tail, :] * eb
        cols = jnp.transpose(jnp.concatenate([ea, eb], axis=0))
        for h in range(heads):
            rows = slice(h * nh, (h + 1) * nh)
            ca = jnp.broadcast_to(cols[:nh, h:h + 1], (nh, 128))
            cb = jnp.broadcast_to(cols[:nh, heads + h:heads + h + 1], (nh, 128))
            for z in range(2):
                mix[g, h // 2, z, (h % 2) * nh:(h % 2 + 1) * nh, :] = a[z, rows, :] * ca + b[z, rows, :] * cb
        for z, ml in enumerate((m, total)):
            for c in range(4):
                rolled = ml if c == 0 else jnp.concatenate([ml[2 * c:], ml[:2 * c]], axis=0)
                mix[g, c, z, 2 * nh:2 * nh + heads, :] = rolled

    def project(g):
        for k in (1, 2, 3):
            one_copy(g, k).wait_recv()
        parts = [mix.at[g, chip]] + [got_1.at[g, k] for k in range(3)]
        tail = slice(2 * nh, 2 * nh + heads)
        peaks = [r[0, tail, :] for r in parts]
        m = functools.reduce(jnp.maximum, peaks)
        es = [jnp.exp(x - m) for x in peaks]
        total = sum(e * r[1, tail, :] for e, r in zip(es, parts))
        total = jnp.where(total > 0, total, 1.0)
        cols = jnp.transpose(jnp.concatenate([e / total for e in es], axis=0))
        outs = []
        for j in range(2):
            cs = [jnp.broadcast_to(cols[:nh, i * heads + j:i * heads + j + 1], (nh, 128)) for i in range(4)]
            o = [sum(r[z, j * nh:(j + 1) * nh, :] * c for r, c in zip(parts, cs)) for z in range(2)]
            outs.append(jnp.concatenate(o, axis=1).astype(BF16))
        for c in range(4):
            w = slice(c * quarter, (c + 1) * quarter)
            yp[g, c] = (jnp.dot(outs[0], wo2[0, :, w], preferred_element_type=F32)
                        + jnp.dot(outs[1], wo2[1, :, w], preferred_element_type=F32))

    def settle(g):
        for k in (1, 2, 3):
            two_copy(g, k).wait_recv()
        y = yp[g, chip] + got_2[g, 0] + got_2[g, 1] + got_2[g, 2]
        ybuf[2 * g + core, :, pl.ds(pl.multiple_of(chip * quarter, quarter), quarter)] = y.astype(BF16)

    keep_w.start()

    def step(it, carry):
        @pl.when(it < groups)
        def _():
            lax.fori_loop(0, 2, lambda half, c: (attend(it, half), c)[1], 0)
            d_copy(it).start()

        @pl.when(jnp.logical_and(it >= 1, it < groups + 1))
        def _():
            merge(it - 1)

        @pl.when(it == LAG_C)
        def _():
            keep_w.wait()
            send_w.wait()

        @pl.when(jnp.logical_and(it >= 1, it < groups + 1))
        def _():
            for k in (3, 1, 2):
                one_copy(it - 1, k).start()

        @pl.when(jnp.logical_and(it >= LAG_C, it < groups + LAG_C))
        def _():
            project(it - LAG_C)
            for k in (3, 1, 2):
                two_copy(it - LAG_C, k).start()

        @pl.when(jnp.logical_and(it >= LAG_S, it < groups + LAG_S))
        def _():
            settle(it - LAG_S)
            for k in (3, 1, 2):
                three_copy(it - LAG_S, k).start()

        @pl.when(it >= LAG_R)
        def _():
            for k in (1, 2, 3):
                three_copy(it - LAG_R, k).wait_recv()
            relay_copy(it - LAG_R).start()
        return carry

    lax.fori_loop(0, groups + LAG_R, step, 0)

    def finish(g, carry):
        relay_copy(g).wait()
        d_copy(g).wait_send()
        for k in (1, 2, 3):
            one_copy(g, k).wait_send()
            two_copy(g, k).wait_send()
            three_copy(g, k).wait_send()
        return carry

    lax.fori_loop(0, groups, finish, 0)
    y_ref[...] = ybuf[...]


def write_kernel(dims, pos_ref, kn_ref, vn_ref, held, k_hbm, v_hbm, ko_hbm, vo_hbm,
                 kc, vc, k_slab, v_slab, sem_in, sem_out, sem_keep, sem_slab):
    n_seq, seq_local, n_blocks, slots = dims
    nh = HALF
    step = nh // 2
    kr, vr = held.at[0], held.at[1]
    lost = n_blocks - slots
    pieces = lost * 2
    row = lax.broadcasted_iota(jnp.int32, (16, kn_ref.shape[1]), 0)

    def owned(b):
        p = pos_ref[b]
        return p, jnp.logical_and(p >= 0, p < seq_local)

    def keep_copies(t):
        s = lax.rem(t, slots)
        rows = pl.ds(t * nh, nh)
        return (pltpu.make_async_copy(kr.at[s], ko_hbm.at[rows], sem_keep.at[0, s]),
                pltpu.make_async_copy(vr.at[s], vo_hbm.at[rows], sem_keep.at[1, s]))

    def in_copies(j):
        rows = pl.ds(j * step, step)
        return (pltpu.make_async_copy(k_hbm.at[rows], kc.at[lax.rem(j, 2)], sem_in.at[0, lax.rem(j, 2)]),
                pltpu.make_async_copy(v_hbm.at[rows], vc.at[lax.rem(j, 2)], sem_in.at[1, lax.rem(j, 2)]))

    def out_copies(j):
        rows = pl.ds(j * step, step)
        return (pltpu.make_async_copy(kc.at[lax.rem(j, 2)], ko_hbm.at[rows], sem_out.at[0, lax.rem(j, 2)]),
                pltpu.make_async_copy(vc.at[lax.rem(j, 2)], vo_hbm.at[rows], sem_out.at[1, lax.rem(j, 2)]))

    def fixed(src, new_ref, b, base, p):
        return jnp.where(row + base == p, new_ref[b].astype(BF16), src)

    for j in range(min(2, pieces)):
        for cp in in_copies(j):
            cp.start()

    def begin(t, c):
        for cp in keep_copies(t):
            cp.start()
        return c

    lax.fori_loop(lost, n_blocks, begin, 0)

    def again(j, c):
        for cp in in_copies(j):
            cp.wait()
        for i in range(step):
            b = j * step + i
            p, own = owned(b)

            @pl.when(own)
            def _():
                base = pl.multiple_of(p // 16 * 16, 16)
                for buf, new_ref in ((kc, kn_ref), (vc, vn_ref)):
                    at = (lax.rem(j, 2), i, pl.ds(base, 16), slice(None))
                    buf[at] = fixed(buf[at], new_ref, b, base, p)
        for cp in out_copies(j):
            cp.start()

        @pl.when(j + 2 < pieces)
        def _():
            for cp in out_copies(j):
                cp.wait()
            for cp in in_copies(j + 2):
                cp.start()
        return c

    lax.fori_loop(0, pieces, again, 0)

    def slab(b, c):
        p, own = owned(b)

        @pl.when(own)
        def _():
            t = b // nh
            base = pl.multiple_of(p // 16 * 16, 16)
            at = (lax.rem(t, slots), lax.rem(b, nh), pl.ds(base, 16), slice(None))
            k_slab[b - lost * nh] = fixed(kr[at], kn_ref, b, base, p)
            v_slab[b - lost * nh] = fixed(vr[at], vn_ref, b, base, p)
        return c

    lax.fori_loop(lost * nh, n_seq, slab, 0)

    def slab_copies(b, p):
        at = pl.ds(pl.multiple_of(p // 16 * 16, 16), 16)
        return (pltpu.make_async_copy(k_slab.at[b - lost * nh], ko_hbm.at[b, at], sem_slab.at[0]),
                pltpu.make_async_copy(v_slab.at[b - lost * nh], vo_hbm.at[b, at], sem_slab.at[1]))

    def patch(t, c):
        for cp in keep_copies(t):
            cp.wait()

        def one(i, c):
            p, own = owned(t * nh + i)

            @pl.when(own)
            def _():
                for cp in slab_copies(t * nh + i, p):
                    cp.start()
            return c
        return lax.fori_loop(0, nh, one, c)

    lax.fori_loop(lost, n_blocks, patch, 0)

    def drain(b, c):
        p, own = owned(b)

        @pl.when(own)
        def _():
            for cp in slab_copies(b, p):
                cp.wait()
        return c

    lax.fori_loop(lost * nh, n_seq, drain, 0)
    for j in range(max(pieces - 2, 0), pieces):
        for cp in out_copies(j):
            cp.wait()


def solution(mesh):
    def local_step(tokens, w_query, w_key, w_value, w_out, k_cache, v_cache, positions):
        n_seq, seq_local, hd = k_cache.shape
        width = w_query.shape[1]
        heads = width // hd
        nh = HALF
        groups = n_seq // (2 * nh)
        n_blocks = 2 * groups
        slots = n_blocks * 3 // 4
        q = jnp.dot(tokens, w_query, preferred_element_type=F32).astype(BF16).reshape(n_seq, heads, hd)
        k_new = jnp.dot(tokens, w_key, preferred_element_type=F32).astype(BF16).astype(F32)
        v_new = jnp.dot(tokens, w_value, preferred_element_type=F32).astype(BF16).astype(F32)
        local_pos = positions - lax.axis_index('sp') * seq_local
        vmem, hbm = pl.BlockSpec(memory_space=pltpu.VMEM), pl.BlockSpec(memory_space=pl.ANY)
        smem = pl.BlockSpec(memory_space=pltpu.SMEM)
        dma = pltpu.SemaphoreType.DMA
        held = pltpu.VMEM((2, slots, nh, seq_local, hd), BF16)
        rows_d, rows_1, quarter = heads * nh + heads, 2 * nh + heads, width // 4
        y, kept = pl.pallas_call(
            functools.partial(attend_kernel, (n_seq, heads, seq_local, hd, groups, slots)),
            out_shape=(jax.ShapeDtypeStruct((n_blocks, nh, width), BF16), held),
            in_specs=[smem, vmem, vmem, vmem, vmem, hbm, hbm],
            out_specs=(vmem, vmem),
            scratch_shapes=[
                pltpu.VMEM((groups, 2, 2, rows_d, 128), F32),
                pltpu.VMEM((groups, 2, rows_d, 128), F32),
                pltpu.VMEM((groups, 4, 2, rows_1, 128), F32),
                pltpu.VMEM((groups, 3, 2, rows_1, 128), F32),
                pltpu.VMEM((groups, 4, nh, quarter), F32),
                pltpu.VMEM((groups, 3, nh, quarter), F32),
                pltpu.VMEM((n_blocks, nh, width), BF16),
                pltpu.VMEM((2,) + w_out.shape, BF16),
                dma((slots,)), dma((slots,)), dma((3,)),
                dma((groups,)), dma((groups,)),
                dma((groups, 3)), dma((groups, 3)),
                dma((groups, 3)), dma((groups, 3)),
                dma((groups, 3)), dma((groups, 3)),
                dma((groups,)), dma((groups,)),
            ],
            compiler_params=pltpu.CompilerParams(collective_id=0, has_side_effects=True,
                                                 vmem_limit_bytes=VMEM_A),
        )(local_pos, q, k_new, v_new, w_out, k_cache, v_cache)
        keep = slots * nh
        k_upd, v_upd = pl.pallas_call(
            functools.partial(write_kernel, (n_seq, seq_local, n_blocks, slots)),
            out_shape=(jax.ShapeDtypeStruct(k_cache.shape, BF16),) * 2,
            in_specs=[smem, vmem, vmem, vmem, hbm, hbm],
            out_specs=(hbm, hbm),
            scratch_shapes=[
                pltpu.VMEM((2, nh // 2, seq_local, hd), BF16), pltpu.VMEM((2, nh // 2, seq_local, hd), BF16),
                pltpu.VMEM((keep, 16, hd), BF16), pltpu.VMEM((keep, 16, hd), BF16),
                dma((2, 2)), dma((2, 2)), dma((2, slots)), dma((2,)),
            ],
            compiler_params=pltpu.CompilerParams(vmem_limit_bytes=VMEM_B),
        )(local_pos, k_new.reshape(n_seq, 1, hd), v_new.reshape(n_seq, 1, hd),
          pltpu.with_memory_space_constraint(kept, pltpu.VMEM), k_cache, v_cache)
        return y.reshape(n_seq, width), k_upd, v_upd

    cache_spec = P('dp', 'sp', None)
    return jax.shard_map(local_step, mesh=mesh, in_specs=(P('dp', None), P(), P(), P(), P('sp', None), cache_spec, cache_spec, P('dp')), out_specs=(P('dp', None), cache_spec, cache_spec), check_vma=False)


VMEM_A = 14 << 20
VMEM_B = 8 << 20
```

```python
import functools

import jax
import jax.numpy as jnp
from jax import lax
from jax.experimental import pallas as pl
from jax.experimental.pallas import tpu as pltpu
from jax.sharding import PartitionSpec as P

MESH = pl.DeviceIdType.MESH
F32, BF16 = jnp.float32, jnp.bfloat16
FLOOR = -1e30
HALF = 16
RING = 4
LAG_C, LAG_S, LAG_R = 3, 5, 7


def attend_kernel(dims, pos_ref, q_ref, kn_ref, vn_ref, wo_ref, k_hbm, v_hbm, y_ref, held,
                  part, got_d, mix, got_1, yp, got_2, ybuf, wo2, sem_k, sem_v, sem_w,
                  snd_d, rcv_d, snd_1, rcv_1, snd_2, rcv_2, snd_3, rcv_3, snd_r, rcv_r):
    n_seq, heads, seq_local, hd, groups, slots = dims
    nh, width = HALF, wo_ref.shape[1]
    kb, vb = held.at[0], held.at[1]
    n_blocks, quarter = 2 * groups, width // 4
    body = heads * nh
    scale = hd ** -0.5
    me = lax.axis_index('sp')
    chip, core = me // 2, lax.rem(me, 2)

    def peer(k):
        return {'sp': jnp.bitwise_xor(me, k)}

    def cache_copies(t):
        s = lax.rem(t, slots)
        rows = pl.ds(t * nh, nh)
        return (pltpu.make_async_copy(k_hbm.at[rows], kb.at[s], sem_k.at[s]),
                pltpu.make_async_copy(v_hbm.at[rows], vb.at[s], sem_v.at[s]))

    def load(t):
        for cp in cache_copies(t):
            cp.start()

    for t in range(min(slots, n_blocks)):
        load(t)

    gate = pltpu.get_barrier_semaphore()
    for k in (1, 2, 4, 6):
        pl.semaphore_signal(gate, inc=1, device_id=peer(k), device_id_type=MESH)
    pl.semaphore_wait(gate, 4)

    send_w = pltpu.make_async_remote_copy(wo_ref, wo2.at[core], sem_w.at[0], sem_w.at[1],
                                          device_id=peer(1), device_id_type=MESH)
    send_w.start()
    keep_w = pltpu.make_async_copy(wo_ref, wo2.at[core], sem_w.at[2])

    def d_copy(g):
        return pltpu.make_async_remote_copy(part.at[g, 1 - core], got_d.at[g], snd_d.at[g], rcv_d.at[g],
                                            device_id=peer(1), device_id_type=MESH)

    def one_copy(g, k):
        return pltpu.make_async_remote_copy(mix.at[g, jnp.bitwise_xor(chip, k)], got_1.at[g, k - 1],
                                            snd_1.at[g, k - 1], rcv_1.at[g, k - 1],
                                            device_id=peer(2 * k), device_id_type=MESH)

    def two_copy(g, k):
        return pltpu.make_async_remote_copy(yp.at[g, jnp.bitwise_xor(chip, k)], got_2.at[g, k - 1],
                                            snd_2.at[g, k - 1], rcv_2.at[g, k - 1],
                                            device_id=peer(2 * k), device_id_type=MESH)

    def three_copy(g, k):
        block = ybuf.at[2 * g + core, :, pl.ds(pl.multiple_of(chip * quarter, quarter), quarter)]
        return pltpu.make_async_remote_copy(block, block, snd_3.at[g, k - 1], rcv_3.at[g, k - 1],
                                            device_id=peer(2 * k), device_id_type=MESH)

    def relay_copy(g):
        rows = ybuf.at[2 * g + core]
        return pltpu.make_async_remote_copy(rows, rows, snd_r.at[g], rcv_r.at[g],
                                            device_id=peer(1), device_id_type=MESH)

    slot_ids = lax.broadcasted_iota(jnp.int32, (heads, seq_local), 1)
    lane = lax.broadcasted_iota(jnp.int32, (heads, 128), 1)

    def attend(g, half):
        t = 2 * g + half
        s = lax.rem(t, slots)
        for cp in cache_copies(t):
            cp.wait()
        first = pl.multiple_of(t * nh, nh)
        kn, vn = kn_ref[pl.ds(first, nh), :].astype(F32), vn_ref[pl.ds(first, nh), :].astype(F32)
        scores = []
        for i in range(nh):
            scores.append(lax.dot_general(q_ref[first + i], kb[s, i], (((1,), (1,)), ((), ())),
                                          preferred_element_type=F32) * scale)
        peaks = jnp.full((heads, 128), FLOOR, F32)
        sums = jnp.zeros((heads, 128), F32)
        weights = []
        for i in range(nh):
            p = pos_ref[first + i]
            own = jnp.logical_and(p >= 0, p < seq_local)
            sc = jnp.where(slot_ids < p, scores[i], -jnp.inf)
            fresh = jnp.sum(q_ref[first + i].astype(F32) * kn[i:i + 1, :], axis=1, keepdims=True) * scale
            fresh = jnp.where(own, fresh, -jnp.inf)
            m = jnp.maximum(jnp.maximum(jnp.max(sc, axis=1, keepdims=True), fresh), FLOOR)
            w, wf = jnp.exp(sc - m), jnp.exp(fresh - m)
            peaks = jnp.where(lane == i, m, peaks)
            sums = jnp.where(lane == i, jnp.sum(w, axis=1, keepdims=True) + wf, sums)
            weights.append((w.astype(BF16), wf.astype(BF16).astype(F32)))
        for i in range(nh):
            w, wf = weights[i]
            o = jnp.dot(w, vb[s, i], preferred_element_type=F32) + wf * vn[i:i + 1, :]
            for z in range(2):
                part[g, half, z, pl.ds(i, heads, stride=nh), :] = o[:, z * 128:(z + 1) * 128]
        part[g, half, 0, body:body + heads, :] = peaks
        part[g, half, 1, body:body + heads, :] = sums

        @pl.when(t + slots < n_blocks)
        def _():
            load(t + slots)

    def merge(g):
        d_copy(g).wait_recv()
        a, b = part.at[g, core], got_d.at[g]
        tail = slice(body, body + heads)
        m = jnp.maximum(a[0, tail, :], b[0, tail, :])
        ea, eb = jnp.exp(a[0, tail, :] - m), jnp.exp(b[0, tail, :] - m)
        total = a[1, tail, :] * ea + b[1, tail, :] * eb
        cols = jnp.transpose(jnp.concatenate([ea, eb], axis=0))
        for h in range(heads):
            rows = slice(h * nh, (h + 1) * nh)
            ca = jnp.broadcast_to(cols[:nh, h:h + 1], (nh, 128))
            cb = jnp.broadcast_to(cols[:nh, heads + h:heads + h + 1], (nh, 128))
            for z in range(2):
                mix[g, h // 2, z, (h % 2) * nh:(h % 2 + 1) * nh, :] = a[z, rows, :] * ca + b[z, rows, :] * cb
        for z, ml in enumerate((m, total)):
            for c in range(4):
                rolled = ml if c == 0 else jnp.concatenate([ml[2 * c:], ml[:2 * c]], axis=0)
                mix[g, c, z, 2 * nh:2 * nh + heads, :] = rolled

    def project(g):
        for k in (1, 2, 3):
            one_copy(g, k).wait_recv()
        parts = [mix.at[g, chip]] + [got_1.at[g, k] for k in range(3)]
        tail = slice(2 * nh, 2 * nh + heads)
        peaks = [r[0, tail, :] for r in parts]
        m = functools.reduce(jnp.maximum, peaks)
        es = [jnp.exp(x - m) for x in peaks]
        total = sum(e * r[1, tail, :] for e, r in zip(es, parts))
        total = jnp.where(total > 0, total, 1.0)
        cols = jnp.transpose(jnp.concatenate([e / total for e in es], axis=0))
        outs = []
        for j in range(2):
            cs = [jnp.broadcast_to(cols[:nh, i * heads + j:i * heads + j + 1], (nh, 128)) for i in range(4)]
            o = [sum(r[z, j * nh:(j + 1) * nh, :] * c for r, c in zip(parts, cs)) for z in range(2)]
            outs.append(jnp.concatenate(o, axis=1).astype(BF16))
        for c in range(4):
            w = slice(c * quarter, (c + 1) * quarter)
            yp[g, c] = (jnp.dot(outs[0], wo2[0, :, w], preferred_element_type=F32)
                        + jnp.dot(outs[1], wo2[1, :, w], preferred_element_type=F32))

    def settle(g):
        for k in (1, 2, 3):
            two_copy(g, k).wait_recv()
        y = yp[g, chip] + got_2[g, 0] + got_2[g, 1] + got_2[g, 2]
        ybuf[2 * g + core, :, pl.ds(pl.multiple_of(chip * quarter, quarter), quarter)] = y.astype(BF16)

    keep_w.start()

    def step(it, carry):
        @pl.when(it < groups)
        def _():
            lax.fori_loop(0, 2, lambda half, c: (attend(it, half), c)[1], 0)
            d_copy(it).start()

        @pl.when(jnp.logical_and(it >= 1, it < groups + 1))
        def _():
            merge(it - 1)

        @pl.when(it == LAG_C)
        def _():
            keep_w.wait()
            send_w.wait()

        @pl.when(jnp.logical_and(it >= 1, it < groups + 1))
        def _():
            for k in (3, 1, 2):
                one_copy(it - 1, k).start()

        @pl.when(jnp.logical_and(it >= LAG_C, it < groups + LAG_C))
        def _():
            project(it - LAG_C)
            for k in (3, 1, 2):
                two_copy(it - LAG_C, k).start()

        @pl.when(jnp.logical_and(it >= LAG_S, it < groups + LAG_S))
        def _():
            settle(it - LAG_S)
            for k in (3, 1, 2):
                three_copy(it - LAG_S, k).start()

        @pl.when(it >= LAG_R)
        def _():
            for k in (1, 2, 3):
                three_copy(it - LAG_R, k).wait_recv()
            relay_copy(it - LAG_R).start()
        return carry

    lax.fori_loop(0, groups + LAG_R, step, 0)

    def finish(g, carry):
        relay_copy(g).wait()
        d_copy(g).wait_send()
        for k in (1, 2, 3):
            one_copy(g, k).wait_send()
            two_copy(g, k).wait_send()
            three_copy(g, k).wait_send()
        return carry

    lax.fori_loop(0, groups, finish, 0)
    y_ref[...] = ybuf[...]


def write_kernel(dims, pos_ref, kn_ref, vn_ref, y_in, _, k_hbm, v_hbm, ko_hbm, vo_hbm, y_hbm, held,
                 kc, vc, sem_in, sem_out, sem_keep, sem_y):
    n_seq, seq_local, n_blocks, slots = dims
    nh = HALF
    step = nh // 2
    lost = n_blocks - slots
    pieces = lost * 2
    row = lax.broadcasted_iota(jnp.int32, (16, kn_ref.shape[-1]), 0)

    def keep_copies(t):
        s = t % slots
        rows = pl.ds(t * nh, nh)
        return (pltpu.make_async_copy(held.at[0, s], ko_hbm.at[rows], sem_keep.at[0, s]),
                pltpu.make_async_copy(held.at[1, s], vo_hbm.at[rows], sem_keep.at[1, s]))

    def in_copies(j):
        rows, r = pl.ds(j * step, step), j % RING
        return (pltpu.make_async_copy(k_hbm.at[rows], kc.at[r], sem_in.at[0, r]),
                pltpu.make_async_copy(v_hbm.at[rows], vc.at[r], sem_in.at[1, r]))

    def out_copies(j):
        rows, r = pl.ds(j * step, step), j % RING
        return (pltpu.make_async_copy(kc.at[r], ko_hbm.at[rows], sem_out.at[0, r]),
                pltpu.make_async_copy(vc.at[r], vo_hbm.at[rows], sem_out.at[1, r]))

    def start(copies):
        for cp in copies:
            cp.start()

    def wait(copies):
        for cp in copies:
            cp.wait()

    def renew(bufs, first, n):
        def one(i, c):
            p = pos_ref[first + i]

            @pl.when(jnp.logical_and(p >= 0, p < seq_local))
            def _():
                base = pl.multiple_of(p // 16 * 16, 16)
                for buf, new_ref in zip(bufs, (kn_ref, vn_ref)):
                    at = (i, pl.ds(base, 16), slice(None))
                    buf[at] = jnp.where(row + base == p, new_ref[first + i].astype(BF16), buf[at])
            return c
        lax.fori_loop(0, n, one, 0)

    y_copy = pltpu.make_async_copy(y_in, y_hbm, sem_y)
    y_copy.start()
    for j in range(min(RING, pieces)):
        start(in_copies(j))
    done = 0
    for j in range(pieces):
        upto = slots * (j + 1) // pieces
        for t in range(lost + done, lost + upto):
            renew((held.at[0, t % slots], held.at[1, t % slots]), t * nh, nh)
        for t in range(lost + done, lost + upto):
            start(keep_copies(t))
        done = upto
        if 1 <= j and j - 1 + RING < pieces:
            wait(out_copies(j - 1))
            start(in_copies(j - 1 + RING))
        wait(in_copies(j))
        renew((kc.at[j % RING], vc.at[j % RING]), j * step, step)
        start(out_copies(j))
    for j in range(max(pieces - RING, 0), pieces):
        wait(out_copies(j))
    for t in range(lost, n_blocks):
        wait(keep_copies(t))
    y_copy.wait()


def solution(mesh):
    def local_step(tokens, w_query, w_key, w_value, w_out, k_cache, v_cache, positions):
        n_seq, seq_local, hd = k_cache.shape
        width = w_query.shape[1]
        heads = width // hd
        nh = HALF
        groups = n_seq // (2 * nh)
        n_blocks = 2 * groups
        slots = n_blocks * 3 // 4
        q = jnp.dot(tokens, w_query, preferred_element_type=F32).astype(BF16).reshape(n_seq, heads, hd)
        k_new = jnp.dot(tokens, w_key, preferred_element_type=F32).astype(BF16)
        v_new = jnp.dot(tokens, w_value, preferred_element_type=F32).astype(BF16)
        local_pos = positions - lax.axis_index('sp') * seq_local
        vmem, hbm = pl.BlockSpec(memory_space=pltpu.VMEM), pl.BlockSpec(memory_space=pl.ANY)
        smem = pl.BlockSpec(memory_space=pltpu.SMEM)
        dma = pltpu.SemaphoreType.DMA
        held = pltpu.VMEM((2, slots, nh, seq_local, hd), BF16)
        rows_d, rows_1, quarter = heads * nh + heads, 2 * nh + heads, width // 4
        y, kept = pl.pallas_call(
            functools.partial(attend_kernel, (n_seq, heads, seq_local, hd, groups, slots)),
            out_shape=(jax.ShapeDtypeStruct((n_blocks, nh, width), BF16), held),
            in_specs=[smem, vmem, vmem, vmem, vmem, hbm, hbm],
            out_specs=(vmem, vmem),
            scratch_shapes=[
                pltpu.VMEM((groups, 2, 2, rows_d, 128), F32),
                pltpu.VMEM((groups, 2, rows_d, 128), F32),
                pltpu.VMEM((groups, 4, 2, rows_1, 128), F32),
                pltpu.VMEM((groups, 3, 2, rows_1, 128), F32),
                pltpu.VMEM((groups, 4, nh, quarter), F32),
                pltpu.VMEM((groups, 3, nh, quarter), F32),
                pltpu.VMEM((n_blocks, nh, width), BF16),
                pltpu.VMEM((2,) + w_out.shape, BF16),
                dma((slots,)), dma((slots,)), dma((3,)),
                dma((groups,)), dma((groups,)),
                dma((groups, 3)), dma((groups, 3)),
                dma((groups, 3)), dma((groups, 3)),
                dma((groups, 3)), dma((groups, 3)),
                dma((groups,)), dma((groups,)),
            ],
            compiler_params=pltpu.CompilerParams(collective_id=0, has_side_effects=True,
                                                 vmem_limit_bytes=VMEM_A),
        )(local_pos, q, k_new, v_new, w_out, k_cache, v_cache)
        k_upd, v_upd, y, _ = pl.pallas_call(
            functools.partial(write_kernel, (n_seq, seq_local, n_blocks, slots)),
            out_shape=(jax.ShapeDtypeStruct(k_cache.shape, BF16),) * 2 + (jax.ShapeDtypeStruct(y.shape, BF16), held),
            in_specs=[smem, vmem, vmem, vmem, vmem, hbm, hbm],
            out_specs=(hbm, hbm, hbm, vmem),
            input_output_aliases={4: 3},
            scratch_shapes=[
                pltpu.VMEM((RING, nh // 2, seq_local, hd), BF16), pltpu.VMEM((RING, nh // 2, seq_local, hd), BF16),
                dma((2, RING)), dma((2, RING)), dma((2, slots)), dma,
            ],
            compiler_params=pltpu.CompilerParams(vmem_limit_bytes=VMEM_B),
        )(local_pos, k_new.astype(F32).reshape(n_seq, 1, hd), v_new.astype(F32).reshape(n_seq, 1, hd), y,
          pltpu.with_memory_space_constraint(kept, pltpu.VMEM), k_cache, v_cache)
        return y.reshape(n_seq, width), k_upd, v_upd

    cache_spec = P('dp', 'sp', None)
    return jax.shard_map(local_step, mesh=mesh, in_specs=(P('dp', None), P(), P(), P(), P('sp', None), cache_spec, cache_spec, P('dp')), out_specs=(P('dp', None), cache_spec, cache_spec), check_vma=False)


VMEM_A = 14 << 20
VMEM_B = 12 << 20
```

```python
import functools

import jax
import jax.numpy as jnp
from jax import lax
from jax.experimental import pallas as pl
from jax.experimental.pallas import tpu as pltpu
from jax.sharding import PartitionSpec as P

MESH = pl.DeviceIdType.MESH
F32, BF16 = jnp.float32, jnp.bfloat16
FLOOR = -1e30
HALF = 16
RING = 4
LAG_C, LAG_S, LAG_R = 3, 5, 7


def attend_kernel(dims, pos_ref, x_ref, wq_hbm, wk_hbm, wv_hbm, wo_hbm, k_hbm, v_hbm,
                  y_ref, held, kn_ref, vn_ref,
                  q_ref, part, got_d, mix, got_1, obuf, wcol, sem_k, sem_v, sem_w, snd_w, rcv_w, snd_v, rcv_v,
                  snd_d, rcv_d, snd_1, rcv_1, snd_2, rcv_2, snd_3, rcv_3, snd_r, rcv_r):
    heads, seq_local, hd, groups, slots = dims
    nh = HALF
    width = wo_hbm.shape[1]
    n_blocks, quarter = 2 * groups, width // 4
    body = heads * nh
    scale = hd ** -0.5
    me = lax.axis_index('sp')
    chip, core = me // 2, lax.rem(me, 2)
    kb, vb = held.at[0], held.at[1]
    n_tiles = heads + 2
    first_stage = slots - pl.cdiv(n_tiles, 4)

    def peer(k):
        return {'sp': jnp.bitwise_xor(me, k)}

    def remote(src, dst, snd, rcv, k):
        return pltpu.make_async_remote_copy(src, dst, snd, rcv, device_id=peer(k), device_id_type=MESH)

    def columns(c):
        return pl.ds(pl.multiple_of(c * quarter, quarter), quarter)

    def cache_copies(t):
        s = lax.rem(t, slots)
        rows = pl.ds(t * nh, nh)
        return (pltpu.make_async_copy(k_hbm.at[rows], kb.at[s], sem_k.at[s]),
                pltpu.make_async_copy(v_hbm.at[rows], vb.at[s], sem_v.at[s]))

    def load(t):
        for cp in cache_copies(t):
            cp.start()

    def staged(w):
        return held.at[lax.rem(w, 4) // 2, first_stage + w // 4, pl.ds(lax.rem(w, 2) * 8, 8)]

    for w in range(n_tiles):
        src = wq_hbm.at[:, :, pl.ds(w * hd, hd)] if w < heads else (wk_hbm, wv_hbm)[w - heads]
        pltpu.make_async_copy(src, staged(w), sem_w.at[w]).start()

    gate = pltpu.get_barrier_semaphore()
    for k in (1, 2, 4, 6):
        pl.semaphore_signal(gate, inc=1, device_id=peer(k), device_id_type=MESH)
    pl.semaphore_wait(gate, 4)

    own_w = pltpu.make_async_copy(wo_hbm.at[:, columns(chip)], wcol.at[me], sem_w.at[n_tiles])

    def cross_w(k):
        return remote(wo_hbm.at[:, columns(jnp.bitwise_xor(chip, k))], wcol.at[me],
                      snd_w.at[k - 1], rcv_w.at[k - 1], 2 * k)

    def relay_w(k):
        src = jnp.bitwise_xor(me, 2 * k)
        return remote(wcol.at[src], wcol.at[src], snd_v.at[k], rcv_v.at[k], 1)

    for k in (3, 1, 2):
        cross_w(k).start()
    own_w.start()

    def d_copy(g):
        return remote(part.at[g, 1 - core], got_d.at[g], snd_d.at[g], rcv_d.at[g], 1)

    def one_copy(g, k):
        return remote(mix.at[g, jnp.bitwise_xor(chip, k)], got_1.at[g, k - 1],
                      snd_1.at[g, k - 1], rcv_1.at[g, k - 1], 2 * k)

    def two_copy(g, k):
        block = obuf.at[g, :, columns(chip)]
        return remote(block, block, snd_2.at[g, k - 1], rcv_2.at[g, k - 1], 2 * k)

    def three_copy(g, k):
        block = y_ref.at[2 * g + core, :, columns(chip)]
        return remote(block, block, snd_3.at[g, k - 1], rcv_3.at[g, k - 1], 2 * k)

    def relay_copy(g):
        rows = y_ref.at[2 * g + core]
        return remote(rows, rows, snd_r.at[g], rcv_r.at[g], 1)

    def tile(w, c):
        pltpu.make_async_copy(wk_hbm, staged(w), sem_w.at[w]).wait()

        @pl.when(w < first_stage)
        def _():
            load(w)
        wt = staged(w)[...].reshape(x_ref.shape[1], hd)
        acc = jnp.dot(x_ref[...], wt, preferred_element_type=F32)

        @pl.when(w < heads)
        def _():
            for z in range(2):
                q_ref[z, pl.ds(w, x_ref.shape[0], stride=heads), :] = acc[:, z * 128:(z + 1) * 128]

        @pl.when(w == heads)
        def _():
            kn_ref[...] = acc.astype(BF16).astype(F32)

        @pl.when(w == heads + 1)
        def _():
            vn_ref[...] = acc.astype(BF16).astype(F32)
        return c

    lax.fori_loop(0, n_tiles, tile, 0)
    for t in range(min(first_stage, n_tiles), slots):
        load(t)

    slot_ids = lax.broadcasted_iota(jnp.int32, (heads, seq_local), 1)
    lane = lax.broadcasted_iota(jnp.int32, (heads, 128), 1)

    def attend(g, half):
        t = 2 * g + half
        s = lax.rem(t, slots)
        for cp in cache_copies(t):
            cp.wait()
        first = pl.multiple_of(t * nh, nh)
        kn, vn = kn_ref[pl.ds(first, nh), :], vn_ref[pl.ds(first, nh), :]
        scores, qs = [], []
        for i in range(nh):
            rows = pl.ds(pl.multiple_of((first + i) * heads, heads), heads)
            q = jnp.concatenate([q_ref[0, rows, :], q_ref[1, rows, :]], axis=1).astype(BF16)
            qs.append(q)
            scores.append(lax.dot_general(q, kb[s, i], (((1,), (1,)), ((), ())), preferred_element_type=F32) * scale)
        peaks = jnp.full((heads, 128), FLOOR, F32)
        sums = jnp.zeros((heads, 128), F32)
        weights = []
        for i in range(nh):
            p = pos_ref[first + i] - me * seq_local
            own = jnp.logical_and(p >= 0, p < seq_local)
            sc = jnp.where(slot_ids < p, scores[i], -jnp.inf)
            fresh = jnp.sum(qs[i].astype(F32) * kn[i:i + 1, :], axis=1, keepdims=True) * scale
            fresh = jnp.where(own, fresh, -jnp.inf)
            m = jnp.maximum(jnp.maximum(jnp.max(sc, axis=1, keepdims=True), fresh), FLOOR)
            w, wf = jnp.exp(sc - m), jnp.exp(fresh - m)
            peaks = jnp.where(lane == i, m, peaks)
            sums = jnp.where(lane == i, jnp.sum(w, axis=1, keepdims=True) + wf, sums)
            weights.append((w.astype(BF16), wf.astype(BF16).astype(F32)))
        for i in range(nh):
            w, wf = weights[i]
            o = jnp.dot(w, vb[s, i], preferred_element_type=F32) + wf * vn[i:i + 1, :]
            for z in range(2):
                part[g, half, z, pl.ds(i, heads, stride=nh), :] = o[:, z * 128:(z + 1) * 128]
        part[g, half, 0, body:body + heads, :] = peaks
        part[g, half, 1, body:body + heads, :] = sums

        @pl.when(t + slots < n_blocks)
        def _():
            load(t + slots)

    def merge(g):
        d_copy(g).wait_recv()
        a, b = part.at[g, core], got_d.at[g]
        tail = slice(body, body + heads)
        m = jnp.maximum(a[0, tail, :], b[0, tail, :])
        ea, eb = jnp.exp(a[0, tail, :] - m), jnp.exp(b[0, tail, :] - m)
        total = a[1, tail, :] * ea + b[1, tail, :] * eb
        cols = jnp.transpose(jnp.concatenate([ea, eb], axis=0))
        for h in range(heads):
            rows = slice(h * nh, (h + 1) * nh)
            ca = jnp.broadcast_to(cols[:nh, h:h + 1], (nh, 128))
            cb = jnp.broadcast_to(cols[:nh, heads + h:heads + h + 1], (nh, 128))
            for z in range(2):
                at = (2 * z + h % 2) * nh
                mix[g, h // 2, at:at + nh, :] = a[z, rows, :] * ca + b[z, rows, :] * cb
        for c in range(4):
            mine = slice(2 * c, 2 * c + 2)
            mix[g, c, 4 * nh:4 * nh + 8, :] = jnp.concatenate([m[mine], total[mine], m[:4]], axis=0)

    def combine(g):
        for k in (1, 2, 3):
            one_copy(g, k).wait_recv()
        parts = [mix.at[g, chip]] + [got_1.at[g, k] for k in range(3)]
        stats = [r[4 * nh:4 * nh + 8, :] for r in parts]
        m = functools.reduce(jnp.maximum, stats)
        es = [jnp.exp(x - m) for x in stats]
        total = sum(e * jnp.concatenate([x[2:], x[:2]], axis=0) for e, x in zip(es, stats))
        total = jnp.where(total > 0, total, 1.0)
        cols = jnp.transpose(jnp.concatenate([e / total for e in es], axis=0))
        outs = []
        for j in range(2):
            cs = [jnp.broadcast_to(cols[:nh, i * 8 + j:i * 8 + j + 1], (nh, 128)) for i in range(4)]
            for z in range(2):
                at = (2 * z + j) * nh
                outs.append(sum(r[at:at + nh, :] * c for r, c in zip(parts, cs)))
        obuf[g, :, columns(chip)] = jnp.concatenate(outs, axis=1).astype(BF16)

    def project(g):
        for k in (1, 2, 3):
            two_copy(g, k).wait_recv()
        y = jnp.dot(obuf[g], wcol[...].reshape(width, quarter), preferred_element_type=F32)
        y_ref[2 * g + core, :, columns(chip)] = y.astype(BF16)

    def step(it, carry):
        @pl.when(it < groups)
        def _():
            lax.fori_loop(0, 2, lambda half, c: (attend(it, half), c)[1], 0)
            d_copy(it).start()

        @pl.when(it == LAG_C)
        def _():
            own_w.wait()
            relay_w(0).start()
            for k in (1, 2, 3):
                cross_w(k).wait()
                relay_w(k).start()

        @pl.when(jnp.logical_and(it >= 1, it < groups + 1))
        def _():
            merge(it - 1)
            for k in (3, 1, 2):
                one_copy(it - 1, k).start()

        @pl.when(jnp.logical_and(it >= LAG_C, it < groups + LAG_C))
        def _():
            combine(it - LAG_C)
            for k in (3, 1, 2):
                two_copy(it - LAG_C, k).start()

        @pl.when(it == LAG_S)
        def _():
            for k in range(4):
                relay_w(k).wait()

        @pl.when(jnp.logical_and(it >= LAG_S, it < groups + LAG_S))
        def _():
            project(it - LAG_S)
            for k in (3, 1, 2):
                three_copy(it - LAG_S, k).start()

        @pl.when(it >= LAG_R)
        def _():
            for k in (1, 2, 3):
                three_copy(it - LAG_R, k).wait_recv()
            relay_copy(it - LAG_R).start()
        return carry

    lax.fori_loop(0, groups + LAG_R, step, 0)

    def finish(g, carry):
        relay_copy(g).wait()
        d_copy(g).wait_send()
        for k in (1, 2, 3):
            one_copy(g, k).wait_send()
            two_copy(g, k).wait_send()
            three_copy(g, k).wait_send()
        return carry

    lax.fori_loop(0, groups, finish, 0)


def write_kernel(dims, pos_ref, kn_ref, vn_ref, y_in, _, k_hbm, v_hbm, ko_hbm, vo_hbm, y_hbm, held,
                 kc, vc, sem_in, sem_out, sem_keep, sem_y):
    n_seq, seq_local, n_blocks, slots = dims
    nh = HALF
    step = nh // 2
    lost = n_blocks - slots
    pieces = lost * 2
    row = lax.broadcasted_iota(jnp.int32, (16, kn_ref.shape[-1]), 0)

    def keep_copies(t):
        s = t % slots
        rows = pl.ds(t * nh, nh)
        return (pltpu.make_async_copy(held.at[0, s], ko_hbm.at[rows], sem_keep.at[0, s]),
                pltpu.make_async_copy(held.at[1, s], vo_hbm.at[rows], sem_keep.at[1, s]))

    def in_copies(j):
        rows, r = pl.ds(j * step, step), j % RING
        return (pltpu.make_async_copy(k_hbm.at[rows], kc.at[r], sem_in.at[0, r]),
                pltpu.make_async_copy(v_hbm.at[rows], vc.at[r], sem_in.at[1, r]))

    def out_copies(j):
        rows, r = pl.ds(j * step, step), j % RING
        return (pltpu.make_async_copy(kc.at[r], ko_hbm.at[rows], sem_out.at[0, r]),
                pltpu.make_async_copy(vc.at[r], vo_hbm.at[rows], sem_out.at[1, r]))

    def start(copies):
        for cp in copies:
            cp.start()

    def wait(copies):
        for cp in copies:
            cp.wait()

    def renew(bufs, first, n):
        def one(i, c):
            p = pos_ref[first + i] - lax.axis_index('sp') * seq_local

            @pl.when(jnp.logical_and(p >= 0, p < seq_local))
            def _():
                base = pl.multiple_of(p // 16 * 16, 16)
                around = pl.ds(pl.multiple_of((first + i) // 8 * 8, 8), 8)
                for buf, new_ref in zip(bufs, (kn_ref, vn_ref)):
                    at = (i, pl.ds(base, 16), slice(None))
                    new = jnp.sum(jnp.where(row[:8] == lax.rem(first + i, 8), new_ref[around, :], 0.0), axis=0, keepdims=True)
                    buf[at] = jnp.where(row + base == p, new.astype(BF16), buf[at])
            return c
        lax.fori_loop(0, n, one, 0)

    y_copy = pltpu.make_async_copy(y_in, y_hbm, sem_y)
    y_copy.start()
    for j in range(min(RING, pieces)):
        start(in_copies(j))
    done = 0
    for j in range(pieces):
        upto = slots * (j + 1) // pieces
        for t in range(lost + done, lost + upto):
            renew((held.at[0, t % slots], held.at[1, t % slots]), t * nh, nh)
        for t in range(lost + done, lost + upto):
            start(keep_copies(t))
        done = upto
        if 1 <= j and j - 1 + RING < pieces:
            wait(out_copies(j - 1))
            start(in_copies(j - 1 + RING))
        wait(in_copies(j))
        renew((kc.at[j % RING], vc.at[j % RING]), j * step, step)
        start(out_copies(j))
    for j in range(max(pieces - RING, 0), pieces):
        wait(out_copies(j))
    for t in range(lost, n_blocks):
        wait(keep_copies(t))
    y_copy.wait()


def solution(mesh):
    def local_step(tokens, w_query, w_key, w_value, w_out, k_cache, v_cache, positions):
        n_seq, seq_local, hd = k_cache.shape
        width = w_query.shape[1]
        heads = width // hd
        nh = HALF
        groups = n_seq // (2 * nh)
        n_blocks = 2 * groups
        slots = n_blocks * 3 // 4
        vmem, hbm = pl.BlockSpec(memory_space=pltpu.VMEM), pl.BlockSpec(memory_space=pl.ANY)
        smem = pl.BlockSpec(memory_space=pltpu.SMEM)
        dma = pltpu.SemaphoreType.DMA
        held = pltpu.VMEM((2, slots, nh, seq_local, hd), BF16)
        rows_d, rows_1 = heads * nh + heads, 4 * nh + 8
        d_model = tokens.shape[1]
        cut = d_model // 8
        n_stage = heads + 3
        y, kept, k_new, v_new = pl.pallas_call(
            functools.partial(attend_kernel, (heads, seq_local, hd, groups, slots)),
            out_shape=(jax.ShapeDtypeStruct((n_blocks, nh, width), BF16), held,
                       jax.ShapeDtypeStruct((n_seq, hd), F32), jax.ShapeDtypeStruct((n_seq, hd), F32)),
            in_specs=[smem, vmem, hbm, hbm, hbm, hbm, hbm, hbm],
            out_specs=(vmem,) * 4,
            scratch_shapes=[
                pltpu.VMEM((2, n_seq * heads, 128), F32),
                pltpu.VMEM((groups, 2, 2, rows_d, 128), F32),
                pltpu.VMEM((groups, 2, rows_d, 128), F32),
                pltpu.VMEM((groups, 4, rows_1, 128), F32),
                pltpu.VMEM((groups, 3, rows_1, 128), F32),
                pltpu.VMEM((groups, nh, width), BF16),
                pltpu.VMEM((heads, w_out.shape[0], width // 4), BF16),
                dma((slots,)), dma((slots,)), dma((n_stage,)),
                dma((3,)), dma((3,)), dma((4,)), dma((4,)),
                dma((groups,)), dma((groups,)),
                dma((groups, 3)), dma((groups, 3)),
                dma((groups, 3)), dma((groups, 3)),
                dma((groups, 3)), dma((groups, 3)),
                dma((groups,)), dma((groups,)),
            ],
            compiler_params=pltpu.CompilerParams(collective_id=0, has_side_effects=True,
                                                 vmem_limit_bytes=VMEM_A),
        )(positions, tokens, w_query.reshape(8, cut, width), w_key.reshape(8, cut, hd), w_value.reshape(8, cut, hd),
          w_out, k_cache, v_cache)
        kept = pltpu.with_memory_space_constraint(kept, pltpu.VMEM)
        k_upd, v_upd, y, _ = pl.pallas_call(
            functools.partial(write_kernel, (n_seq, seq_local, n_blocks, slots)),
            out_shape=(jax.ShapeDtypeStruct(k_cache.shape, BF16),) * 2 + (jax.ShapeDtypeStruct(y.shape, BF16), held),
            in_specs=[smem, vmem, vmem, vmem, vmem, hbm, hbm],
            out_specs=(hbm, hbm, hbm, vmem),
            input_output_aliases={4: 3},
            scratch_shapes=[
                pltpu.VMEM((RING, nh // 2, seq_local, hd), BF16), pltpu.VMEM((RING, nh // 2, seq_local, hd), BF16),
                dma((2, RING)), dma((2, RING)), dma((2, slots)), dma,
            ],
            compiler_params=pltpu.CompilerParams(vmem_limit_bytes=VMEM_B),
        )(positions, k_new, v_new, y, kept, k_cache, v_cache)
        return y.reshape(n_seq, width), k_upd, v_upd

    cache_spec = P('dp', 'sp', None)
    return jax.shard_map(local_step, mesh=mesh, in_specs=(P('dp', None), P(), P(), P(), P('sp', None), cache_spec, cache_spec, P('dp')), out_specs=(P('dp', None), cache_spec, cache_spec), check_vma=False)


VMEM_A = 14 << 20
VMEM_B = 12 << 20
```

```python
import functools

import jax
import jax.numpy as jnp
from jax import lax
from jax.experimental import pallas as pl
from jax.experimental.pallas import tpu as pltpu
from jax.sharding import PartitionSpec as P

MESH = pl.DeviceIdType.MESH
F32, BF16 = jnp.float32, jnp.bfloat16
FLOOR = -1e30
HALF = 16
RING = 4
LAG_C, LAG_S, LAG_R, LAG_Y = 4, 7, 10, 12


def attend_kernel(dims, pos_ref, x_hbm, wq_hbm, wk_hbm, wv_hbm, wo_hbm, k_hbm, v_hbm,
                  y_hbm, held, kn_hbm, vn_hbm,
                  x_ref, y_ref, kn_ref, vn_ref, q_ref, part, got_d, mix, got_1, obuf, wcol, sem_k, sem_v, sem_w, snd_w, rcv_w, snd_v, rcv_v,
                  snd_d, rcv_d, snd_1, rcv_1, snd_2, rcv_2, snd_3, rcv_3, snd_r, rcv_r, sem_y):
    heads, seq_local, hd, groups, slots = dims
    nh = HALF
    width = wo_hbm.shape[1]
    n_blocks, quarter = 2 * groups, width // 4
    body = heads * nh
    scale = hd ** -0.5
    me = lax.axis_index('sp')
    chip, core = me // 2, lax.rem(me, 2)
    kb, vb = held.at[0], held.at[1]
    n_tiles = heads + 2
    first_stage = slots - pl.cdiv(n_tiles, 4)

    def peer(k):
        return {'sp': jnp.bitwise_xor(me, k)}

    def remote(src, dst, snd, rcv, k):
        return pltpu.make_async_remote_copy(src, dst, snd, rcv, device_id=peer(k), device_id_type=MESH)

    def columns(c):
        return pl.ds(pl.multiple_of(c * quarter, quarter), quarter)

    def cache_copies(t):
        s = lax.rem(t, slots)
        rows = pl.ds(t * nh, nh)
        return (pltpu.make_async_copy(k_hbm.at[rows], kb.at[s], sem_k.at[s]),
                pltpu.make_async_copy(v_hbm.at[rows], vb.at[s], sem_v.at[s]))

    def load(t):
        for cp in cache_copies(t):
            cp.start()

    def staged(w):
        return held.at[lax.rem(w, 4) // 2, first_stage + w // 4, pl.ds(lax.rem(w, 2) * 8, 8)]

    x_copy = pltpu.make_async_copy(x_hbm, x_ref, sem_w.at[n_tiles + 1])
    x_copy.start()
    for w in range(n_tiles):
        src = wq_hbm.at[:, :, pl.ds(w * hd, hd)] if w < heads else (wk_hbm, wv_hbm)[w - heads]
        pltpu.make_async_copy(src, staged(w), sem_w.at[w]).start()

    gate = pltpu.get_barrier_semaphore()
    for k in (1, 2, 4, 6):
        pl.semaphore_signal(gate, inc=1, device_id=peer(k), device_id_type=MESH)
    pl.semaphore_wait(gate, 4)

    own_w = pltpu.make_async_copy(wo_hbm.at[:, columns(chip)], wcol.at[me], sem_w.at[n_tiles])

    def cross_w(k):
        return remote(wo_hbm.at[:, columns(jnp.bitwise_xor(chip, k))], wcol.at[me],
                      snd_w.at[k - 1], rcv_w.at[k - 1], 2 * k)

    def relay_w(k):
        src = jnp.bitwise_xor(me, 2 * k)
        return remote(wcol.at[src], wcol.at[src], snd_v.at[k], rcv_v.at[k], 1)

    for k in (3, 1, 2):
        cross_w(k).start()
    own_w.start()

    def d_copy(g):
        return remote(part.at[g, 1 - core], got_d.at[g], snd_d.at[g], rcv_d.at[g], 1)

    def one_copy(g, k):
        return remote(mix.at[g, jnp.bitwise_xor(chip, k)], got_1.at[g, k - 1],
                      snd_1.at[g, k - 1], rcv_1.at[g, k - 1], 2 * k)

    def two_copy(g, k):
        block = obuf.at[g, :, columns(chip)]
        return remote(block, block, snd_2.at[g, k - 1], rcv_2.at[g, k - 1], 2 * k)

    def three_copy(g, k):
        block = y_ref.at[2 * g + core, :, columns(chip)]
        return remote(block, block, snd_3.at[g, k - 1], rcv_3.at[g, k - 1], 2 * k)

    def relay_copy(g):
        rows = y_ref.at[2 * g + core]
        return remote(rows, rows, snd_r.at[g], rcv_r.at[g], 1)

    def y_copy(g):
        rows = pl.ds(2 * g, 2)
        return pltpu.make_async_copy(y_ref.at[rows], y_hbm.at[rows], sem_y.at[g])

    def tile(w, c):
        pltpu.make_async_copy(wk_hbm, staged(w), sem_w.at[w]).wait()

        @pl.when(w < first_stage)
        def _():
            load(w)
        wt = staged(w)[...].reshape(x_ref.shape[1], hd)
        acc = jnp.dot(x_ref[...], wt, preferred_element_type=F32)

        @pl.when(w < heads)
        def _():
            for z in range(2):
                q_ref[z, pl.ds(w, x_ref.shape[0], stride=heads), :] = acc[:, z * 128:(z + 1) * 128]

        @pl.when(w == heads)
        def _():
            kn_ref[...] = acc.astype(BF16).astype(F32)

        @pl.when(w == heads + 1)
        def _():
            vn_ref[...] = acc.astype(BF16).astype(F32)
        return c

    x_copy.wait()
    lax.fori_loop(0, n_tiles, tile, 0)
    kn_out = pltpu.make_async_copy(kn_ref, kn_hbm, sem_w.at[n_tiles])
    vn_out = pltpu.make_async_copy(vn_ref, vn_hbm, sem_w.at[n_tiles + 1])
    for t in range(min(first_stage, n_tiles), slots):
        load(t)

    slot_ids = lax.broadcasted_iota(jnp.int32, (heads, seq_local), 1)
    lane = lax.broadcasted_iota(jnp.int32, (heads, 128), 1)

    def attend(g, half):
        t = 2 * g + half
        s = lax.rem(t, slots)
        for cp in cache_copies(t):
            cp.wait()
        first = pl.multiple_of(t * nh, nh)
        kn, vn = kn_ref[pl.ds(first, nh), :], vn_ref[pl.ds(first, nh), :]
        scores, qs = [], []
        for i in range(nh):
            rows = pl.ds(pl.multiple_of((first + i) * heads, heads), heads)
            q = jnp.concatenate([q_ref[0, rows, :], q_ref[1, rows, :]], axis=1).astype(BF16)
            qs.append(q)
            scores.append(lax.dot_general(q, kb[s, i], (((1,), (1,)), ((), ())), preferred_element_type=F32) * scale)
        peaks = jnp.full((heads, 128), FLOOR, F32)
        sums = jnp.zeros((heads, 128), F32)
        weights = []
        for i in range(nh):
            p = pos_ref[first + i] - me * seq_local
            own = jnp.logical_and(p >= 0, p < seq_local)
            sc = jnp.where(slot_ids < p, scores[i], -jnp.inf)
            fresh = jnp.sum(qs[i].astype(F32) * kn[i:i + 1, :], axis=1, keepdims=True) * scale
            fresh = jnp.where(own, fresh, -jnp.inf)
            m = jnp.maximum(jnp.maximum(jnp.max(sc, axis=1, keepdims=True), fresh), FLOOR)
            w, wf = jnp.exp(sc - m), jnp.exp(fresh - m)
            peaks = jnp.where(lane == i, m, peaks)
            sums = jnp.where(lane == i, jnp.sum(w, axis=1, keepdims=True) + wf, sums)
            weights.append((w.astype(BF16), wf.astype(BF16).astype(F32)))
        for i in range(nh):
            w, wf = weights[i]
            o = jnp.dot(w, vb[s, i], preferred_element_type=F32) + wf * vn[i:i + 1, :]
            for z in range(2):
                part[g, half, z, pl.ds(i, heads, stride=nh), :] = o[:, z * 128:(z + 1) * 128]
        part[g, half, 0, body:body + heads, :] = peaks
        part[g, half, 1, body:body + heads, :] = sums

        @pl.when(t + slots < n_blocks)
        def _():
            load(t + slots)

    def merge(g):
        d_copy(g).wait_recv()
        a, b = part.at[g, core], got_d.at[g]
        tail = slice(body, body + heads)
        m = jnp.maximum(a[0, tail, :], b[0, tail, :])
        ea, eb = jnp.exp(a[0, tail, :] - m), jnp.exp(b[0, tail, :] - m)
        total = a[1, tail, :] * ea + b[1, tail, :] * eb
        cols = jnp.transpose(jnp.concatenate([ea, eb], axis=0))
        for h in range(heads):
            rows = slice(h * nh, (h + 1) * nh)
            ca = jnp.broadcast_to(cols[:nh, h:h + 1], (nh, 128))
            cb = jnp.broadcast_to(cols[:nh, heads + h:heads + h + 1], (nh, 128))
            for z in range(2):
                at = (2 * z + h % 2) * nh
                mix[g, h // 2, at:at + nh, :] = a[z, rows, :] * ca + b[z, rows, :] * cb
        for c in range(4):
            mine = slice(2 * c, 2 * c + 2)
            mix[g, c, 4 * nh:4 * nh + 8, :] = jnp.concatenate([m[mine], total[mine], m[:4]], axis=0)

    def combine(g):
        for k in (1, 2, 3):
            one_copy(g, k).wait_recv()
        parts = [mix.at[g, chip]] + [got_1.at[g, k] for k in range(3)]
        stats = [r[4 * nh:4 * nh + 8, :] for r in parts]
        m = functools.reduce(jnp.maximum, stats)
        es = [jnp.exp(x - m) for x in stats]
        total = sum(e * jnp.concatenate([x[2:], x[:2]], axis=0) for e, x in zip(es, stats))
        total = jnp.where(total > 0, total, 1.0)
        cols = jnp.transpose(jnp.concatenate([e / total for e in es], axis=0))
        outs = []
        for j in range(2):
            cs = [jnp.broadcast_to(cols[:nh, i * 8 + j:i * 8 + j + 1], (nh, 128)) for i in range(4)]
            for z in range(2):
                at = (2 * z + j) * nh
                outs.append(sum(r[at:at + nh, :] * c for r, c in zip(parts, cs)))
        obuf[g, :, columns(chip)] = jnp.concatenate(outs, axis=1).astype(BF16)

    def project(g):
        for k in (1, 2, 3):
            two_copy(g, k).wait_recv()
        y = jnp.dot(obuf[g], wcol[...].reshape(width, quarter), preferred_element_type=F32)
        y_ref[2 * g + core, :, columns(chip)] = y.astype(BF16)

    def step(it, carry):
        @pl.when(it < groups)
        def _():
            lax.fori_loop(0, 2, lambda half, c: (attend(it, half), c)[1], 0)
            d_copy(it).start()

        @pl.when(it == LAG_C)
        def _():
            own_w.wait()
            kn_out.start()
            vn_out.start()
            relay_w(0).start()
            for k in (1, 2, 3):
                cross_w(k).wait()
                relay_w(k).start()

        @pl.when(jnp.logical_and(it >= 1, it < groups + 1))
        def _():
            merge(it - 1)
            for k in (3, 1, 2):
                one_copy(it - 1, k).start()

        @pl.when(jnp.logical_and(it >= LAG_C, it < groups + LAG_C))
        def _():
            combine(it - LAG_C)
            for k in (3, 1, 2):
                two_copy(it - LAG_C, k).start()

        @pl.when(it == LAG_S)
        def _():
            for k in range(4):
                relay_w(k).wait()

        @pl.when(jnp.logical_and(it >= LAG_S, it < groups + LAG_S))
        def _():
            project(it - LAG_S)
            for k in (3, 1, 2):
                three_copy(it - LAG_S, k).start()

        @pl.when(jnp.logical_and(it >= LAG_R, it < groups + LAG_R))
        def _():
            for k in (1, 2, 3):
                three_copy(it - LAG_R, k).wait_recv()
            relay_copy(it - LAG_R).start()

        @pl.when(it >= LAG_Y)
        def _():
            relay_copy(it - LAG_Y).wait_recv()
            y_copy(it - LAG_Y).start()
        return carry

    lax.fori_loop(0, groups + LAG_Y, step, 0)
    kn_out.wait()
    vn_out.wait()

    def finish(g, carry):
        relay_copy(g).wait_send()
        y_copy(g).wait()
        d_copy(g).wait_send()
        for k in (1, 2, 3):
            one_copy(g, k).wait_send()
            two_copy(g, k).wait_send()
            three_copy(g, k).wait_send()
        return carry

    lax.fori_loop(0, groups, finish, 0)


def write_kernel(dims, pos_ref, kn_hbm, vn_hbm, y_in, _, k_hbm, v_hbm, ko_hbm, vo_hbm, y_hbm, held,
                 kn_ref, vn_ref, y_ref, kc, vc, sem_in, sem_out, sem_keep, sem_y):
    n_seq, seq_local, n_blocks, slots = dims
    nh = HALF
    step = nh // 2
    lost = n_blocks - slots
    pieces = lost * 2
    row = lax.broadcasted_iota(jnp.int32, (16, kn_ref.shape[-1]), 0)

    def keep_copies(t):
        s = t % slots
        rows = pl.ds(t * nh, nh)
        return (pltpu.make_async_copy(held.at[0, s], ko_hbm.at[rows], sem_keep.at[0, s]),
                pltpu.make_async_copy(held.at[1, s], vo_hbm.at[rows], sem_keep.at[1, s]))

    def in_copies(j):
        rows, r = pl.ds(j * step, step), j % RING
        return (pltpu.make_async_copy(k_hbm.at[rows], kc.at[r], sem_in.at[0, r]),
                pltpu.make_async_copy(v_hbm.at[rows], vc.at[r], sem_in.at[1, r]))

    def out_copies(j):
        rows, r = pl.ds(j * step, step), j % RING
        return (pltpu.make_async_copy(kc.at[r], ko_hbm.at[rows], sem_out.at[0, r]),
                pltpu.make_async_copy(vc.at[r], vo_hbm.at[rows], sem_out.at[1, r]))

    def start(copies):
        for cp in copies:
            cp.start()

    def wait(copies):
        for cp in copies:
            cp.wait()

    def renew(bufs, first, n):
        def one(i, c):
            p = pos_ref[first + i] - lax.axis_index('sp') * seq_local

            @pl.when(jnp.logical_and(p >= 0, p < seq_local))
            def _():
                base = pl.multiple_of(p // 16 * 16, 16)
                around = pl.ds(pl.multiple_of((first + i) // 8 * 8, 8), 8)
                for buf, new_ref in zip(bufs, (kn_ref, vn_ref)):
                    at = (i, pl.ds(base, 16), slice(None))
                    new = jnp.sum(jnp.where(row[:8] == lax.rem(first + i, 8), new_ref[around, :], 0.0), axis=0, keepdims=True)
                    buf[at] = jnp.where(row + base == p, new.astype(BF16), buf[at])
            return c
        lax.fori_loop(0, n, one, 0)

    new_copies = (pltpu.make_async_copy(kn_hbm, kn_ref, sem_y.at[0]), pltpu.make_async_copy(vn_hbm, vn_ref, sem_y.at[1]))
    start(new_copies)
    for j in range(min(RING, pieces)):
        start(in_copies(j))
    y_take = pltpu.make_async_copy(y_in, y_ref, sem_y.at[2])
    y_copy = pltpu.make_async_copy(y_ref, y_hbm, sem_y.at[2])
    y_take.start()
    wait(new_copies)
    done = 0
    for j in range(pieces):
        upto = slots * (j + 1) // pieces
        for t in range(lost + done, lost + upto):
            renew((held.at[0, t % slots], held.at[1, t % slots]), t * nh, nh)
        for t in range(lost + done, lost + upto):
            start(keep_copies(t))
        done = upto
        if 1 <= j and j - 1 + RING < pieces:
            wait(out_copies(j - 1))
            start(in_copies(j - 1 + RING))
        wait(in_copies(j))
        renew((kc.at[j % RING], vc.at[j % RING]), j * step, step)
        start(out_copies(j))
        if j == pieces // 2:
            y_take.wait()
            y_copy.start()
    for j in range(max(pieces - RING, 0), pieces):
        wait(out_copies(j))
    for t in range(lost, n_blocks):
        wait(keep_copies(t))
    y_copy.wait()


def solution(mesh):
    def local_step(tokens, w_query, w_key, w_value, w_out, k_cache, v_cache, positions):
        n_seq, seq_local, hd = k_cache.shape
        width = w_query.shape[1]
        heads = width // hd
        nh = HALF
        groups = n_seq // (2 * nh)
        n_blocks = 2 * groups
        slots = n_blocks * 3 // 4
        vmem, hbm = pl.BlockSpec(memory_space=pltpu.VMEM), pl.BlockSpec(memory_space=pl.ANY)
        smem = pl.BlockSpec(memory_space=pltpu.SMEM)
        dma = pltpu.SemaphoreType.DMA
        held = pltpu.VMEM((2, slots, nh, seq_local, hd), BF16)
        rows_d, rows_1 = heads * nh + heads, 4 * nh + 8
        d_model = tokens.shape[1]
        cut = d_model // 8
        n_stage = heads + 4
        y, kept, k_new, v_new = pl.pallas_call(
            functools.partial(attend_kernel, (heads, seq_local, hd, groups, slots)),
            out_shape=(jax.ShapeDtypeStruct((n_blocks, nh, width), BF16), held,
                       jax.ShapeDtypeStruct((n_seq, hd), F32), jax.ShapeDtypeStruct((n_seq, hd), F32)),
            in_specs=[smem] + [hbm] * 7,
            out_specs=(hbm, vmem, hbm, hbm),
            scratch_shapes=[
                pltpu.VMEM(tokens.shape, BF16), pltpu.VMEM((n_blocks, nh, width), BF16),
                pltpu.VMEM((n_seq, hd), F32), pltpu.VMEM((n_seq, hd), F32),
                pltpu.VMEM((2, n_seq * heads, 128), F32),
                pltpu.VMEM((groups, 2, 2, rows_d, 128), F32),
                pltpu.VMEM((groups, 2, rows_d, 128), F32),
                pltpu.VMEM((groups, 4, rows_1, 128), F32),
                pltpu.VMEM((groups, 3, rows_1, 128), F32),
                pltpu.VMEM((groups, nh, width), BF16),
                pltpu.VMEM((heads, w_out.shape[0], width // 4), BF16),
                dma((slots,)), dma((slots,)), dma((n_stage,)),
                dma((3,)), dma((3,)), dma((4,)), dma((4,)),
                dma((groups,)), dma((groups,)),
                dma((groups, 3)), dma((groups, 3)),
                dma((groups, 3)), dma((groups, 3)),
                dma((groups, 3)), dma((groups, 3)),
                dma((groups,)), dma((groups,)), dma((groups,)),
            ],
            compiler_params=pltpu.CompilerParams(collective_id=0, has_side_effects=True,
                                                 vmem_limit_bytes=VMEM_A),
        )(positions, tokens, w_query.reshape(8, cut, width), w_key.reshape(8, cut, hd), w_value.reshape(8, cut, hd),
          w_out, k_cache, v_cache)
        kept = pltpu.with_memory_space_constraint(kept, pltpu.VMEM)
        k_upd, v_upd, y, _ = pl.pallas_call(
            functools.partial(write_kernel, (n_seq, seq_local, n_blocks, slots)),
            out_shape=(jax.ShapeDtypeStruct(k_cache.shape, BF16),) * 2 + (jax.ShapeDtypeStruct(y.shape, BF16), held),
            in_specs=[smem, hbm, hbm, hbm, vmem, hbm, hbm],
            out_specs=(hbm, hbm, hbm, vmem),
            input_output_aliases={4: 3},
            scratch_shapes=[
                pltpu.VMEM((n_seq, hd), F32), pltpu.VMEM((n_seq, hd), F32), pltpu.VMEM(y.shape, BF16),
                pltpu.VMEM((RING, nh // 2, seq_local, hd), BF16), pltpu.VMEM((RING, nh // 2, seq_local, hd), BF16),
                dma((2, RING)), dma((2, RING)), dma((2, slots)), dma((3,)),
            ],
            compiler_params=pltpu.CompilerParams(vmem_limit_bytes=VMEM_B),
        )(positions, k_new, v_new, y, kept, k_cache, v_cache)
        return y.reshape(n_seq, width), k_upd, v_upd

    cache_spec = P('dp', 'sp', None)
    return jax.shard_map(local_step, mesh=mesh, in_specs=(P('dp', None), P(), P(), P(), P('sp', None), cache_spec, cache_spec, P('dp')), out_specs=(P('dp', None), cache_spec, cache_spec), check_vma=False)


VMEM_A = 14 << 20
VMEM_B = 12 << 20
```

```python
import functools

import jax
import jax.numpy as jnp
from jax import lax
from jax.experimental import pallas as pl
from jax.experimental.pallas import tpu as pltpu
from jax.sharding import PartitionSpec as P

MESH = pl.DeviceIdType.MESH
F32, BF16 = jnp.float32, jnp.bfloat16
FLOOR = -1e30
HALF = 16
RING = 4
DIRECT = 1
LAG_C, LAG_S, LAG_R, LAG_Y = 4, 7, 10, 12


def attend_kernel(dims, pos_ref, x_hbm, wq_hbm, wk_hbm, wv_hbm, wo_hbm, k_hbm, v_hbm,
                  y_hbm, held, kn_hbm, vn_hbm,
                  y_ref, kn_ref, vn_ref, q_ref, part, got_d, mix, got_1, obuf, wcol, sem_k, sem_v, sem_w, snd_w, rcv_w, snd_v, rcv_v,
                  snd_d, rcv_d, snd_1, rcv_1, snd_2, rcv_2, snd_3, rcv_3, snd_r, rcv_r, sem_y, sem_x):
    heads, seq_local, hd, groups, slots = dims
    nh = HALF
    width = wo_hbm.shape[1]
    n_blocks, quarter = 2 * groups, width // 4
    body = heads * nh
    scale = hd ** -0.5
    me = lax.axis_index('sp')
    chip, core = me // 2, lax.rem(me, 2)
    kb, vb = held.at[0], held.at[1]
    n_tiles = heads + 2
    first_stage = slots - pl.cdiv(n_tiles, 4)

    def peer(k):
        return {'sp': jnp.bitwise_xor(me, k)}

    def remote(src, dst, snd, rcv, k):
        return pltpu.make_async_remote_copy(src, dst, snd, rcv, device_id=peer(k), device_id_type=MESH)

    def columns(c):
        return pl.ds(pl.multiple_of(c * quarter, quarter), quarter)

    def cache_copies(t):
        s = lax.rem(t, slots)
        rows = pl.ds(t * nh, nh)
        return (pltpu.make_async_copy(k_hbm.at[rows], kb.at[s], sem_k.at[s]),
                pltpu.make_async_copy(v_hbm.at[rows], vb.at[s], sem_v.at[s]))

    def load(t):
        for cp in cache_copies(t):
            cp.start()

    def staged(w):
        return held.at[lax.rem(w, 4) // 2, first_stage + w // 4, pl.ds(lax.rem(w, 2) * 8, 8)]

    rows_x = x_hbm.shape[0]
    x_cuts = [held.at[1, slots - 1, i] for i in range(8)]
    x_copies = [pltpu.make_async_copy(x_hbm.at[:, pl.ds(i * hd, hd)], x_cuts[i], sem_x.at[i]) for i in range(8)]
    for cp in x_copies:
        cp.start()
    for w in range(n_tiles):
        src = wq_hbm.at[:, :, pl.ds(w * hd, hd)] if w < heads else (wk_hbm, wv_hbm)[w - heads]
        pltpu.make_async_copy(src, staged(w), sem_w.at[w]).start()

    gate = pltpu.get_barrier_semaphore()
    for k in range(1, 8):
        pl.semaphore_signal(gate, inc=1, device_id=peer(k), device_id_type=MESH)
    pl.semaphore_wait(gate, 7)

    own_w = pltpu.make_async_copy(wo_hbm.at[:, columns(chip)], wcol.at[me], sem_w.at[n_tiles])

    def cross_w(k):
        return remote(wo_hbm.at[:, columns(jnp.bitwise_xor(chip, k))], wcol.at[me],
                      snd_w.at[k - 1], rcv_w.at[k - 1], 2 * k)

    def relay_w(k):
        src = jnp.bitwise_xor(me, 2 * k)
        return remote(wcol.at[src], wcol.at[src], snd_v.at[k], rcv_v.at[k], 1)

    for k in (3, 1, 2):
        cross_w(k).start()
    own_w.start()

    def d_copy(g):
        return remote(part.at[g, 1 - core], got_d.at[g], snd_d, rcv_d.at[g], 1)

    def one_copy(g, k):
        return remote(mix.at[g, jnp.bitwise_xor(chip, k)], got_1.at[g, k - 1],
                      snd_1, rcv_1.at[g], 2 * k)

    def two_copy(g, k):
        block = obuf.at[g, :, columns(chip)]
        return remote(block, block, snd_2, rcv_2.at[g], 2 * k)

    def three_copy(g, k):
        block = y_ref.at[2 * g + core, :, columns(chip)]
        return remote(block, block, snd_3, rcv_3.at[g], 2 * k)

    def far_copy(g, k):
        block = y_ref.at[2 * g + core, :, columns(chip)]
        return remote(block, block, snd_r, rcv_r.at[g], 2 * k + 1)

    def relay_copy(g):
        rows = y_ref.at[2 * g + core]
        return remote(rows, rows, snd_r, rcv_r.at[g], 1)

    def y_copy(g):
        rows = pl.ds(2 * g, 2)
        return pltpu.make_async_copy(y_ref.at[rows], y_hbm.at[rows], sem_y)

    def tile(w, c):
        pltpu.make_async_copy(wk_hbm, staged(w), sem_w.at[w]).wait()

        @pl.when(w < first_stage)
        def _():
            load(w)
        wt = staged(w)
        acc = sum(jnp.dot(x_cuts[i][...], wt[i], preferred_element_type=F32) for i in range(8))

        @pl.when(w < heads)
        def _():
            for z in range(2):
                q_ref[z, pl.ds(w, rows_x, stride=heads), :] = acc[:, z * 128:(z + 1) * 128]

        @pl.when(w == heads)
        def _():
            kn_ref[...] = acc.astype(BF16).astype(F32)

        @pl.when(w == heads + 1)
        def _():
            vn_ref[...] = acc.astype(BF16).astype(F32)
        return c

    for cp in x_copies:
        cp.wait()
    lax.fori_loop(0, n_tiles, tile, 0)
    kn_out = pltpu.make_async_copy(kn_ref, kn_hbm, sem_w.at[n_tiles])
    vn_out = pltpu.make_async_copy(vn_ref, vn_hbm, sem_w.at[n_tiles + 1])
    for t in range(min(first_stage, n_tiles), slots):
        load(t)

    slot_ids = lax.broadcasted_iota(jnp.int32, (heads, seq_local), 1)
    lane = lax.broadcasted_iota(jnp.int32, (heads, 128), 1)

    def attend(g, half):
        t = 2 * g + half
        s = lax.rem(t, slots)
        for cp in cache_copies(t):
            cp.wait()
        first = pl.multiple_of(t * nh, nh)
        kn, vn = kn_ref[pl.ds(first, nh), :], vn_ref[pl.ds(first, nh), :]
        scores, qs = [], []
        for i in range(nh):
            rows = pl.ds(pl.multiple_of((first + i) * heads, heads), heads)
            q = jnp.concatenate([q_ref[0, rows, :], q_ref[1, rows, :]], axis=1).astype(BF16)
            qs.append(q)
            scores.append(lax.dot_general(q, kb[s, i], (((1,), (1,)), ((), ())), preferred_element_type=F32) * scale)
        peaks = jnp.full((heads, 128), FLOOR, F32)
        sums = jnp.zeros((heads, 128), F32)
        weights = []
        for i in range(nh):
            p = pos_ref[first + i] - me * seq_local
            own = jnp.logical_and(p >= 0, p < seq_local)
            sc = jnp.where(slot_ids < p, scores[i], -jnp.inf)
            fresh = jnp.sum(qs[i].astype(F32) * kn[i:i + 1, :], axis=1, keepdims=True) * scale
            fresh = jnp.where(own, fresh, -jnp.inf)
            m = jnp.maximum(jnp.maximum(jnp.max(sc, axis=1, keepdims=True), fresh), FLOOR)
            w, wf = jnp.exp(sc - m), jnp.exp(fresh - m)
            peaks = jnp.where(lane == i, m, peaks)
            sums = jnp.where(lane == i, jnp.sum(w, axis=1, keepdims=True) + wf, sums)
            weights.append((w.astype(BF16), wf.astype(BF16).astype(F32)))
        for i in range(nh):
            w, wf = weights[i]
            o = jnp.dot(w, vb[s, i], preferred_element_type=F32) + wf * vn[i:i + 1, :]
            for z in range(2):
                part[g, half, z, pl.ds(i, heads, stride=nh), :] = o[:, z * 128:(z + 1) * 128]
        part[g, half, 0, body:body + heads, :] = peaks
        part[g, half, 1, body:body + heads, :] = sums

        @pl.when(t + slots < n_blocks)
        def _():
            load(t + slots)

    def merge(g):
        d_copy(g).wait_recv()
        a, b = part.at[g, core], got_d.at[g]
        tail = slice(body, body + heads)
        m = jnp.maximum(a[0, tail, :], b[0, tail, :])
        ea, eb = jnp.exp(a[0, tail, :] - m), jnp.exp(b[0, tail, :] - m)
        total = a[1, tail, :] * ea + b[1, tail, :] * eb
        cols = jnp.transpose(jnp.concatenate([ea, eb], axis=0))
        for h in range(heads):
            rows = slice(h * nh, (h + 1) * nh)
            ca = jnp.broadcast_to(cols[:nh, h:h + 1], (nh, 128))
            cb = jnp.broadcast_to(cols[:nh, heads + h:heads + h + 1], (nh, 128))
            for z in range(2):
                at = (2 * z + h % 2) * nh
                mix[g, h // 2, at:at + nh, :] = a[z, rows, :] * ca + b[z, rows, :] * cb
        for c in range(4):
            mine = slice(2 * c, 2 * c + 2)
            mix[g, c, 4 * nh:4 * nh + 8, :] = jnp.concatenate([m[mine], total[mine], m[:4]], axis=0)

    def combine(g):
        remote(got_1.at[g], got_1.at[g], snd_1, rcv_1.at[g], 2).wait_recv()
        parts = [mix.at[g, chip]] + [got_1.at[g, k] for k in range(3)]
        stats = [r[4 * nh:4 * nh + 8, :] for r in parts]
        m = functools.reduce(jnp.maximum, stats)
        es = [jnp.exp(x - m) for x in stats]
        total = sum(e * jnp.concatenate([x[2:], x[:2]], axis=0) for e, x in zip(es, stats))
        total = jnp.where(total > 0, total, 1.0)
        cols = jnp.transpose(jnp.concatenate([e / total for e in es], axis=0))
        outs = []
        for j in range(2):
            cs = [jnp.broadcast_to(cols[:nh, i * 8 + j:i * 8 + j + 1], (nh, 128)) for i in range(4)]
            for z in range(2):
                at = (2 * z + j) * nh
                outs.append(sum(r[at:at + nh, :] * c for r, c in zip(parts, cs)))
        obuf[g, :, columns(chip)] = jnp.concatenate(outs, axis=1).astype(BF16)

    def project(g):
        three = obuf.at[g, :, pl.ds(0, 3 * quarter)]
        remote(three, three, snd_2, rcv_2.at[g], 2).wait_recv()
        y = jnp.dot(obuf[g], wcol[...].reshape(width, quarter), preferred_element_type=F32)
        y_ref[2 * g + core, :, columns(chip)] = y.astype(BF16)

    def step(it, carry):
        @pl.when(it < groups)
        def _():
            lax.fori_loop(0, 2, lambda half, c: (attend(it, half), c)[1], 0)
            d_copy(it).start()

        @pl.when(it == LAG_C)
        def _():
            own_w.wait()
            kn_out.start()
            vn_out.start()
            relay_w(0).start()
            for k in (1, 2, 3):
                cross_w(k).wait()
                relay_w(k).start()

        @pl.when(jnp.logical_and(it >= 1, it < groups + 1))
        def _():
            merge(it - 1)
            for k in (3, 1, 2):
                one_copy(it - 1, k).start()

        @pl.when(jnp.logical_and(it >= LAG_C, it < groups + LAG_C))
        def _():
            combine(it - LAG_C)
            for k in (3, 1, 2):
                two_copy(it - LAG_C, k).start()

        @pl.when(it == LAG_S)
        def _():
            for k in range(4):
                relay_w(k).wait()

        @pl.when(jnp.logical_and(it >= LAG_S, it < groups + LAG_S))
        def _():
            project(it - LAG_S)
            for k in (3, 1, 2):
                three_copy(it - LAG_S, k).start()

            @pl.when(it - LAG_S >= groups - DIRECT)
            def _():
                for k in (3, 1, 2, 0):
                    far_copy(it - LAG_S, k).start()

        @pl.when(jnp.logical_and(it >= LAG_R, it < groups + LAG_R))
        def _():
            three = y_ref.at[2 * (it - LAG_R) + core, :, pl.ds(0, 3 * quarter)]
            remote(three, three, snd_3, rcv_3.at[it - LAG_R], 2).wait_recv()

            @pl.when(it - LAG_R < groups - DIRECT)
            def _():
                relay_copy(it - LAG_R).start()

        @pl.when(it >= LAG_Y)
        def _():
            relay_copy(it - LAG_Y).wait_recv()
            y_copy(it - LAG_Y).start()
        return carry

    lax.fori_loop(0, groups + LAG_Y, step, 0)
    kn_out.wait()
    vn_out.wait()

    blocks = pl.ds(0, 3)
    for sent, sem in ((part.at[:, 0], snd_d), (mix.at[:, blocks], snd_1),
                      (obuf.at[:, :, pl.ds(0, 3 * quarter)], snd_2),
                      (y_ref.at[pl.ds(0, groups), :, pl.ds(0, 3 * quarter)], snd_3),
                      (y_ref.at[pl.ds(0, groups)], snd_r)):
        remote(sent, sent, sem, rcv_d.at[0], 1).wait_send()
    pltpu.make_async_copy(y_ref, y_hbm, sem_y).wait()


def write_kernel(dims, pos_ref, kn_hbm, vn_hbm, y_in, _, k_hbm, v_hbm, ko_hbm, vo_hbm, y_hbm, held,
                 kn_ref, vn_ref, y_ref, kc, vc, sem_in, sem_out, sem_keep, sem_y):
    n_seq, seq_local, n_blocks, slots = dims
    nh = HALF
    step = nh // 2
    lost = n_blocks - slots
    pieces = lost * 2
    row = lax.broadcasted_iota(jnp.int32, (16, kn_ref.shape[-1]), 0)

    def keep_copies(t):
        s = t % slots
        rows = pl.ds(t * nh, nh)
        return (pltpu.make_async_copy(held.at[0, s], ko_hbm.at[rows], sem_keep.at[0, s]),
                pltpu.make_async_copy(held.at[1, s], vo_hbm.at[rows], sem_keep.at[1, s]))

    def in_copies(j):
        rows, r = pl.ds(j * step, step), j % RING
        return (pltpu.make_async_copy(k_hbm.at[rows], kc.at[r], sem_in.at[0, r]),
                pltpu.make_async_copy(v_hbm.at[rows], vc.at[r], sem_in.at[1, r]))

    def out_copies(j):
        rows, r = pl.ds(j * step, step), j % RING
        return (pltpu.make_async_copy(kc.at[r], ko_hbm.at[rows], sem_out.at[0, r]),
                pltpu.make_async_copy(vc.at[r], vo_hbm.at[rows], sem_out.at[1, r]))

    def start(copies):
        for cp in copies:
            cp.start()

    def wait(copies):
        for cp in copies:
            cp.wait()

    def renew(bufs, first, n):
        def one(i, c):
            p = pos_ref[first + i] - lax.axis_index('sp') * seq_local

            @pl.when(jnp.logical_and(p >= 0, p < seq_local))
            def _():
                base = pl.multiple_of(p // 16 * 16, 16)
                around = pl.ds(pl.multiple_of((first + i) // 8 * 8, 8), 8)
                for buf, new_ref in zip(bufs, (kn_ref, vn_ref)):
                    at = (i, pl.ds(base, 16), slice(None))
                    new = jnp.sum(jnp.where(row[:8] == lax.rem(first + i, 8), new_ref[around, :], 0.0), axis=0, keepdims=True)
                    buf[at] = jnp.where(row + base == p, new.astype(BF16), buf[at])
            return c
        lax.fori_loop(0, n, one, 0)

    new_copies = (pltpu.make_async_copy(kn_hbm, kn_ref, sem_y.at[0]), pltpu.make_async_copy(vn_hbm, vn_ref, sem_y.at[1]))
    start(new_copies)
    for j in range(min(RING, pieces)):
        start(in_copies(j))
    y_take = pltpu.make_async_copy(y_in, y_ref, sem_y.at[2])
    y_copy = pltpu.make_async_copy(y_ref, y_hbm, sem_y.at[2])
    y_take.start()
    wait(new_copies)
    done = 0
    for j in range(pieces):
        upto = slots * (j + 1) // pieces
        for t in range(lost + done, lost + upto):
            renew((held.at[0, t % slots], held.at[1, t % slots]), t * nh, nh)
        for t in range(lost + done, lost + upto):
            start(keep_copies(t))
        done = upto
        if 1 <= j and j - 1 + RING < pieces:
            wait(out_copies(j - 1))
            start(in_copies(j - 1 + RING))
        wait(in_copies(j))
        renew((kc.at[j % RING], vc.at[j % RING]), j * step, step)
        start(out_copies(j))
        if j == pieces // 2:
            y_take.wait()
            y_copy.start()
    for j in range(max(pieces - RING, 0), pieces):
        wait(out_copies(j))
    for t in range(lost, n_blocks):
        wait(keep_copies(t))
    y_copy.wait()


def solution(mesh):
    def local_step(tokens, w_query, w_key, w_value, w_out, k_cache, v_cache, positions):
        n_seq, seq_local, hd = k_cache.shape
        width = w_query.shape[1]
        heads = width // hd
        nh = HALF
        groups = n_seq // (2 * nh)
        n_blocks = 2 * groups
        slots = n_blocks * 13 // 16
        vmem, hbm = pl.BlockSpec(memory_space=pltpu.VMEM), pl.BlockSpec(memory_space=pl.ANY)
        smem = pl.BlockSpec(memory_space=pltpu.SMEM)
        dma = pltpu.SemaphoreType.DMA
        held = pltpu.VMEM((2, slots, nh, seq_local, hd), BF16)
        rows_d, rows_1 = heads * nh + heads, 4 * nh + 8
        d_model = tokens.shape[1]
        cut = d_model // 8
        n_stage = heads + 4
        y, kept, k_new, v_new = pl.pallas_call(
            functools.partial(attend_kernel, (heads, seq_local, hd, groups, slots)),
            out_shape=(jax.ShapeDtypeStruct((n_blocks, nh, width), BF16), held,
                       jax.ShapeDtypeStruct((n_seq, hd), F32), jax.ShapeDtypeStruct((n_seq, hd), F32)),
            in_specs=[smem] + [hbm] * 7,
            out_specs=(hbm, vmem, hbm, hbm),
            scratch_shapes=[
                pltpu.VMEM((n_blocks, nh, width), BF16),
                pltpu.VMEM((n_seq, hd), F32), pltpu.VMEM((n_seq, hd), F32),
                pltpu.VMEM((2, n_seq * heads, 128), F32),
                pltpu.VMEM((groups, 2, 2, rows_d, 128), F32),
                pltpu.VMEM((groups, 2, rows_d, 128), F32),
                pltpu.VMEM((groups, 4, rows_1, 128), F32),
                pltpu.VMEM((groups, 3, rows_1, 128), F32),
                pltpu.VMEM((groups, nh, width), BF16),
                pltpu.VMEM((heads, w_out.shape[0], width // 4), BF16),
                dma((slots,)), dma((slots,)), dma((n_stage,)),
                dma((3,)), dma((3,)), dma((4,)), dma((4,)),
                dma, dma((groups,)), dma, dma((groups,)), dma, dma((groups,)), dma, dma((groups,)),
                dma, dma((groups,)), dma, dma((8,)),
            ],
            compiler_params=pltpu.CompilerParams(collective_id=0, has_side_effects=True,
                                                 vmem_limit_bytes=VMEM_A),
        )(positions, tokens, w_query.reshape(8, cut, width), w_key.reshape(8, cut, hd), w_value.reshape(8, cut, hd),
          w_out, k_cache, v_cache)
        kept = pltpu.with_memory_space_constraint(kept, pltpu.VMEM)
        k_upd, v_upd, y, _ = pl.pallas_call(
            functools.partial(write_kernel, (n_seq, seq_local, n_blocks, slots)),
            out_shape=(jax.ShapeDtypeStruct(k_cache.shape, BF16),) * 2 + (jax.ShapeDtypeStruct(y.shape, BF16), held),
            in_specs=[smem, hbm, hbm, hbm, vmem, hbm, hbm],
            out_specs=(hbm, hbm, hbm, vmem),
            input_output_aliases={4: 3},
            scratch_shapes=[
                pltpu.VMEM((n_seq, hd), F32), pltpu.VMEM((n_seq, hd), F32), pltpu.VMEM(y.shape, BF16),
                pltpu.VMEM((RING, nh // 2, seq_local, hd), BF16), pltpu.VMEM((RING, nh // 2, seq_local, hd), BF16),
                dma((2, RING)), dma((2, RING)), dma((2, slots)), dma((3,)),
            ],
            compiler_params=pltpu.CompilerParams(vmem_limit_bytes=VMEM_B),
        )(positions, k_new, v_new, y, kept, k_cache, v_cache)
        return y.reshape(n_seq, width), k_upd, v_upd

    cache_spec = P('dp', 'sp', None)
    return jax.shard_map(local_step, mesh=mesh, in_specs=(P('dp', None), P(), P(), P(), P('sp', None), cache_spec, cache_spec, P('dp')), out_specs=(P('dp', None), cache_spec, cache_spec), check_vma=False)


VMEM_A = int(11.6 * 2**20)
VMEM_B = 10 << 20
```

```python
import functools

import jax
import jax.numpy as jnp
from jax import lax
from jax.experimental import pallas as pl
from jax.experimental.pallas import tpu as pltpu
from jax.sharding import PartitionSpec as P

MESH = pl.DeviceIdType.MESH
F32, BF16 = jnp.float32, jnp.bfloat16
FLOOR = -1e30
HALF = 16
RING = 4
DIRECT = 1
LAG_C, LAG_S, LAG_R, LAG_Y = 3, 6, 9, 10


def attend_kernel(dims, pos_ref, x_hbm, wq_hbm, wk_hbm, wv_hbm, wo_hbm, k_hbm, v_hbm,
                  y_hbm, held, kn_hbm, vn_hbm,
                  y_ref, kn_ref, vn_ref, q_ref, part, got_d, mix, got_1, obuf, wcol, sem_k, sem_v, sem_w, snd_w, rcv_w, snd_v, rcv_v,
                  snd_d, rcv_d, snd_1, rcv_1, snd_2, rcv_2, snd_3, rcv_3, snd_r, rcv_r, sem_y, sem_x):
    heads, seq_local, hd, groups, slots = dims
    nh = HALF
    width = wo_hbm.shape[1]
    n_blocks, quarter = 2 * groups, width // 4
    body = heads * nh
    scale = hd ** -0.5
    me = lax.axis_index('sp')
    chip, core = me // 2, lax.rem(me, 2)
    kb, vb = held.at[0], held.at[1]
    n_tiles = heads + 2
    first_stage = slots - pl.cdiv(n_tiles, 4)

    def peer(k):
        return {'sp': jnp.bitwise_xor(me, k)}

    def remote(src, dst, snd, rcv, k):
        return pltpu.make_async_remote_copy(src, dst, snd, rcv, device_id=peer(k), device_id_type=MESH)

    def columns(c):
        return pl.ds(pl.multiple_of(c * quarter, quarter), quarter)

    def cache_copies(t):
        s = lax.rem(t, slots)
        rows = pl.ds(t * nh, nh)
        return (pltpu.make_async_copy(k_hbm.at[rows], kb.at[s], sem_k.at[s]),
                pltpu.make_async_copy(v_hbm.at[rows], vb.at[s], sem_v.at[s]))

    def load(t):
        for cp in cache_copies(t):
            cp.start()

    def staged(w):
        return held.at[lax.rem(w, 4) // 2, first_stage + w // 4, pl.ds(lax.rem(w, 2) * 8, 8)]

    rows_x = x_hbm.shape[0]
    x_cuts = [held.at[1, slots - 1, i] for i in range(8)]
    x_copies = [pltpu.make_async_copy(x_hbm.at[:, pl.ds(i * hd, hd)], x_cuts[i], sem_x.at[i]) for i in range(8)]
    for cp in x_copies:
        cp.start()
    for w in range(n_tiles):
        src = wq_hbm.at[:, :, pl.ds(w * hd, hd)] if w < heads else (wk_hbm, wv_hbm)[w - heads]
        pltpu.make_async_copy(src, staged(w), sem_w.at[w]).start()

    gate = pltpu.get_barrier_semaphore()
    for k in range(1, 8):
        pl.semaphore_signal(gate, inc=1, device_id=peer(k), device_id_type=MESH)
    pl.semaphore_wait(gate, 7)

    own_w = pltpu.make_async_copy(wo_hbm.at[:, columns(chip)], wcol.at[me], sem_w.at[n_tiles])

    def cross_w(k):
        return remote(wo_hbm.at[:, columns(jnp.bitwise_xor(chip, k))], wcol.at[me],
                      snd_w.at[k - 1], rcv_w.at[k - 1], 2 * k)

    def relay_w(k):
        src = jnp.bitwise_xor(me, 2 * k)
        return remote(wcol.at[src], wcol.at[src], snd_v.at[k], rcv_v.at[k], 1)

    for k in (3, 1, 2):
        cross_w(k).start()
    own_w.start()

    def d_copy(g):
        return remote(part.at[g, 1 - core], got_d.at[g], snd_d, rcv_d.at[g], 1)

    def one_copy(g, k):
        return remote(mix.at[g, jnp.bitwise_xor(chip, k)], got_1.at[g, k - 1],
                      snd_1, rcv_1.at[g], 2 * k)

    def two_copy(g, k):
        block = obuf.at[g, :, columns(chip)]
        return remote(block, block, snd_2, rcv_2.at[g], 2 * k)

    def three_copy(g, k):
        block = y_ref.at[2 * g + core, :, columns(chip)]
        return remote(block, block, snd_3, rcv_3.at[g], 2 * k)

    def far_copy(g, k):
        block = y_ref.at[2 * g + core, :, columns(chip)]
        return remote(block, block, snd_r, rcv_r.at[g], 2 * k + 1)

    def relay_copy(g):
        rows = y_ref.at[2 * g + core]
        return remote(rows, rows, snd_r, rcv_r.at[g], 1)

    def y_copy(g):
        rows = pl.ds(2 * g, 2)
        return pltpu.make_async_copy(y_ref.at[rows], y_hbm.at[rows], sem_y)

    def tile(w, c):
        pltpu.make_async_copy(wk_hbm, staged(w), sem_w.at[w]).wait()

        @pl.when(w < first_stage)
        def _():
            load(w)
        wt = staged(w)
        acc = sum(jnp.dot(x_cuts[i][...], wt[i], preferred_element_type=F32) for i in range(8))

        @pl.when(w < heads)
        def _():
            for z in range(2):
                q_ref[z, pl.ds(w, rows_x, stride=heads), :] = acc[:, z * 128:(z + 1) * 128]

        @pl.when(w == heads)
        def _():
            kn_ref[...] = acc.astype(BF16).astype(F32)

        @pl.when(w == heads + 1)
        def _():
            vn_ref[...] = acc.astype(BF16).astype(F32)
        return c

    for cp in x_copies:
        cp.wait()
    lax.fori_loop(0, n_tiles, tile, 0)
    kn_out = pltpu.make_async_copy(kn_ref, kn_hbm, sem_w.at[n_tiles])
    vn_out = pltpu.make_async_copy(vn_ref, vn_hbm, sem_w.at[n_tiles + 1])
    for t in range(min(first_stage, n_tiles), slots):
        load(t)

    slot_ids = lax.broadcasted_iota(jnp.int32, (heads, seq_local), 1)
    lane = lax.broadcasted_iota(jnp.int32, (heads, 128), 1)

    def attend(g, half):
        t = 2 * g + half
        s = lax.rem(t, slots)
        for cp in cache_copies(t):
            cp.wait()
        first = pl.multiple_of(t * nh, nh)
        kn, vn = kn_ref[pl.ds(first, nh), :], vn_ref[pl.ds(first, nh), :]
        scores, qs = [], []
        for i in range(nh):
            rows = pl.ds(pl.multiple_of((first + i) * heads, heads), heads)
            q = jnp.concatenate([q_ref[0, rows, :], q_ref[1, rows, :]], axis=1).astype(BF16)
            qs.append(q)
            scores.append(lax.dot_general(q, kb[s, i], (((1,), (1,)), ((), ())), preferred_element_type=F32) * scale)
        peaks = jnp.full((heads, 128), FLOOR, F32)
        sums = jnp.zeros((heads, 128), F32)
        weights = []
        for i in range(nh):
            p = pos_ref[first + i] - me * seq_local
            own = jnp.logical_and(p >= 0, p < seq_local)
            sc = jnp.where(slot_ids < p, scores[i], -jnp.inf)
            fresh = jnp.sum(qs[i].astype(F32) * kn[i:i + 1, :], axis=1, keepdims=True) * scale
            fresh = jnp.where(own, fresh, -jnp.inf)
            m = jnp.maximum(jnp.maximum(jnp.max(sc, axis=1, keepdims=True), fresh), FLOOR)
            w, wf = jnp.exp(sc - m), jnp.exp(fresh - m)
            peaks = jnp.where(lane == i, m, peaks)
            sums = jnp.where(lane == i, jnp.sum(w, axis=1, keepdims=True) + wf, sums)
            weights.append((w.astype(BF16), wf.astype(BF16).astype(F32)))
        for i in range(nh):
            w, wf = weights[i]
            o = jnp.dot(w, vb[s, i], preferred_element_type=F32) + wf * vn[i:i + 1, :]
            for z in range(2):
                part[g, half, z, pl.ds(i, heads, stride=nh), :] = o[:, z * 128:(z + 1) * 128]
        part[g, half, 0, body:body + heads, :] = peaks
        part[g, half, 1, body:body + heads, :] = sums

        @pl.when(t + slots < n_blocks)
        def _():
            load(t + slots)

    def merge(g):
        d_copy(g).wait_recv()
        a, b = part.at[g, core], got_d.at[g]
        tail = slice(body, body + heads)
        m = jnp.maximum(a[0, tail, :], b[0, tail, :])
        ea, eb = jnp.exp(a[0, tail, :] - m), jnp.exp(b[0, tail, :] - m)
        total = a[1, tail, :] * ea + b[1, tail, :] * eb
        cols = jnp.transpose(jnp.concatenate([ea, eb], axis=0))
        for h in range(heads):
            rows = slice(h * nh, (h + 1) * nh)
            ca = jnp.broadcast_to(cols[:nh, h:h + 1], (nh, 128))
            cb = jnp.broadcast_to(cols[:nh, heads + h:heads + h + 1], (nh, 128))
            for z in range(2):
                at = (2 * z + h % 2) * nh
                mix[g, h // 2, at:at + nh, :] = a[z, rows, :] * ca + b[z, rows, :] * cb
        for c in range(4):
            mine = slice(2 * c, 2 * c + 2)
            mix[g, c, 4 * nh:4 * nh + 8, :] = jnp.concatenate([m[mine], total[mine], m[:4]], axis=0)

    def combine(g):
        remote(got_1.at[g], got_1.at[g], snd_1, rcv_1.at[g], 2).wait_recv()
        parts = [mix.at[g, chip]] + [got_1.at[g, k] for k in range(3)]
        stats = [r[4 * nh:4 * nh + 8, :] for r in parts]
        m = functools.reduce(jnp.maximum, stats)
        es = [jnp.exp(x - m) for x in stats]
        total = sum(e * jnp.concatenate([x[2:], x[:2]], axis=0) for e, x in zip(es, stats))
        total = jnp.where(total > 0, total, 1.0)
        cols = jnp.transpose(jnp.concatenate([e / total for e in es], axis=0))
        outs = []
        for j in range(2):
            cs = [jnp.broadcast_to(cols[:nh, i * 8 + j:i * 8 + j + 1], (nh, 128)) for i in range(4)]
            for z in range(2):
                at = (2 * z + j) * nh
                outs.append(sum(r[at:at + nh, :] * c for r, c in zip(parts, cs)))
        obuf[g, :, columns(chip)] = jnp.concatenate(outs, axis=1).astype(BF16)

    def project(g):
        three = obuf.at[g, :, pl.ds(0, 3 * quarter)]
        remote(three, three, snd_2, rcv_2.at[g], 2).wait_recv()
        y = jnp.dot(obuf[g], wcol[...].reshape(width, quarter), preferred_element_type=F32)
        y_ref[2 * g + core, :, columns(chip)] = y.astype(BF16)

    def step(it, carry):
        @pl.when(it < groups)
        def _():
            lax.fori_loop(0, 2, lambda half, c: (attend(it, half), c)[1], 0)
            d_copy(it).start()

        @pl.when(it == LAG_C)
        def _():
            own_w.wait()
            kn_out.start()
            vn_out.start()
            relay_w(0).start()
            for k in (1, 2, 3):
                cross_w(k).wait()
                relay_w(k).start()

        @pl.when(jnp.logical_and(it >= 1, it < groups + 1))
        def _():
            merge(it - 1)
            for k in (3, 1, 2):
                one_copy(it - 1, k).start()

        @pl.when(jnp.logical_and(it >= LAG_C, it < groups + LAG_C))
        def _():
            combine(it - LAG_C)
            for k in (3, 1, 2):
                two_copy(it - LAG_C, k).start()

        @pl.when(it == LAG_S)
        def _():
            for k in range(4):
                relay_w(k).wait()

        @pl.when(jnp.logical_and(it >= LAG_S, it < groups + LAG_S))
        def _():
            project(it - LAG_S)
            for k in (3, 1, 2):
                three_copy(it - LAG_S, k).start()

            @pl.when(it - LAG_S >= groups - DIRECT)
            def _():
                for k in (3, 1, 2, 0):
                    far_copy(it - LAG_S, k).start()

        @pl.when(jnp.logical_and(it >= LAG_R, it < groups + LAG_R))
        def _():
            three = y_ref.at[2 * (it - LAG_R) + core, :, pl.ds(0, 3 * quarter)]
            remote(three, three, snd_3, rcv_3.at[it - LAG_R], 2).wait_recv()

            @pl.when(it - LAG_R < groups - DIRECT)
            def _():
                relay_copy(it - LAG_R).start()

        @pl.when(it >= LAG_Y)
        def _():
            relay_copy(it - LAG_Y).wait_recv()
            y_copy(it - LAG_Y).start()
        return carry

    lax.fori_loop(0, groups + LAG_Y, step, 0)
    kn_out.wait()
    vn_out.wait()

    blocks = pl.ds(0, 3)
    for sent, sem in ((part.at[:, 0], snd_d), (mix.at[:, blocks], snd_1),
                      (obuf.at[:, :, pl.ds(0, 3 * quarter)], snd_2),
                      (y_ref.at[pl.ds(0, groups), :, pl.ds(0, 3 * quarter)], snd_3),
                      (y_ref.at[pl.ds(0, groups)], snd_r)):
        remote(sent, sent, sem, rcv_d.at[0], 1).wait_send()
    pltpu.make_async_copy(y_ref, y_hbm, sem_y).wait()


def write_kernel(dims, pos_ref, kn_hbm, vn_hbm, y_in, _, k_hbm, v_hbm, ko_hbm, vo_hbm, y_hbm, held,
                 kn_ref, vn_ref, y_ref, kc, vc, sem_in, sem_out, sem_keep, sem_y):
    n_seq, seq_local, n_blocks, slots = dims
    nh = HALF
    step = nh // 2
    lost = n_blocks - slots
    pieces = lost * 2
    row = lax.broadcasted_iota(jnp.int32, (16, kn_ref.shape[-1]), 0)

    def keep_copies(t):
        s = t % slots
        rows = pl.ds(t * nh, nh)
        return (pltpu.make_async_copy(held.at[0, s], ko_hbm.at[rows], sem_keep.at[0, s]),
                pltpu.make_async_copy(held.at[1, s], vo_hbm.at[rows], sem_keep.at[1, s]))

    def in_copies(j):
        rows, r = pl.ds(j * step, step), j % RING
        return (pltpu.make_async_copy(k_hbm.at[rows], kc.at[r], sem_in.at[0, r]),
                pltpu.make_async_copy(v_hbm.at[rows], vc.at[r], sem_in.at[1, r]))

    def out_copies(j):
        rows, r = pl.ds(j * step, step), j % RING
        return (pltpu.make_async_copy(kc.at[r], ko_hbm.at[rows], sem_out.at[0, r]),
                pltpu.make_async_copy(vc.at[r], vo_hbm.at[rows], sem_out.at[1, r]))

    def start(copies):
        for cp in copies:
            cp.start()

    def wait(copies):
        for cp in copies:
            cp.wait()

    def renew(bufs, first, n):
        def one(i, c):
            p = pos_ref[first + i] - lax.axis_index('sp') * seq_local

            @pl.when(jnp.logical_and(p >= 0, p < seq_local))
            def _():
                base = pl.multiple_of(p // 16 * 16, 16)
                around = pl.ds(pl.multiple_of((first + i) // 8 * 8, 8), 8)
                for buf, new_ref in zip(bufs, (kn_ref, vn_ref)):
                    at = (i, pl.ds(base, 16), slice(None))
                    new = jnp.sum(jnp.where(row[:8] == lax.rem(first + i, 8), new_ref[around, :], 0.0), axis=0, keepdims=True)
                    buf[at] = jnp.where(row + base == p, new.astype(BF16), buf[at])
            return c
        lax.fori_loop(0, n, one, 0)

    new_copies = (pltpu.make_async_copy(kn_hbm, kn_ref, sem_y.at[0]), pltpu.make_async_copy(vn_hbm, vn_ref, sem_y.at[1]))
    start(new_copies)
    for j in range(min(RING, pieces)):
        start(in_copies(j))
    y_take = pltpu.make_async_copy(y_in, y_ref, sem_y.at[2])
    y_copy = pltpu.make_async_copy(y_ref, y_hbm, sem_y.at[2])
    y_take.start()
    wait(new_copies)
    done = 0
    for j in range(pieces):
        upto = slots * (j + 1) // pieces
        for t in range(lost + done, lost + upto):
            renew((held.at[0, t % slots], held.at[1, t % slots]), t * nh, nh)
        for t in range(lost + done, lost + upto):
            start(keep_copies(t))
        done = upto
        if 1 <= j and j - 1 + RING < pieces:
            wait(out_copies(j - 1))
            start(in_copies(j - 1 + RING))
        wait(in_copies(j))
        renew((kc.at[j % RING], vc.at[j % RING]), j * step, step)
        start(out_copies(j))
        if j == pieces // 2:
            y_take.wait()
            y_copy.start()
    for j in range(max(pieces - RING, 0), pieces):
        wait(out_copies(j))
    for t in range(lost, n_blocks):
        wait(keep_copies(t))
    y_copy.wait()


def solution(mesh):
    def local_step(tokens, w_query, w_key, w_value, w_out, k_cache, v_cache, positions):
        n_seq, seq_local, hd = k_cache.shape
        width = w_query.shape[1]
        heads = width // hd
        nh = HALF
        groups = n_seq // (2 * nh)
        n_blocks = 2 * groups
        slots = n_blocks * 13 // 16
        vmem, hbm = pl.BlockSpec(memory_space=pltpu.VMEM), pl.BlockSpec(memory_space=pl.ANY)
        smem = pl.BlockSpec(memory_space=pltpu.SMEM)
        dma = pltpu.SemaphoreType.DMA
        held = pltpu.VMEM((2, slots, nh, seq_local, hd), BF16)
        rows_d, rows_1 = heads * nh + heads, 4 * nh + 8
        d_model = tokens.shape[1]
        cut = d_model // 8
        n_stage = heads + 4
        y, kept, k_new, v_new = pl.pallas_call(
            functools.partial(attend_kernel, (heads, seq_local, hd, groups, slots)),
            out_shape=(jax.ShapeDtypeStruct((n_blocks, nh, width), BF16), held,
                       jax.ShapeDtypeStruct((n_seq, hd), F32), jax.ShapeDtypeStruct((n_seq, hd), F32)),
            in_specs=[smem] + [hbm] * 7,
            out_specs=(hbm, vmem, hbm, hbm),
            scratch_shapes=[
                pltpu.VMEM((n_blocks, nh, width), BF16),
                pltpu.VMEM((n_seq, hd), F32), pltpu.VMEM((n_seq, hd), F32),
                pltpu.VMEM((2, n_seq * heads, 128), F32),
                pltpu.VMEM((groups, 2, 2, rows_d, 128), F32),
                pltpu.VMEM((groups, 2, rows_d, 128), F32),
                pltpu.VMEM((groups, 4, rows_1, 128), F32),
                pltpu.VMEM((groups, 3, rows_1, 128), F32),
                pltpu.VMEM((groups, nh, width), BF16),
                pltpu.VMEM((heads, w_out.shape[0], width // 4), BF16),
                dma((slots,)), dma((slots,)), dma((n_stage,)),
                dma((3,)), dma((3,)), dma((4,)), dma((4,)),
                dma, dma((groups,)), dma, dma((groups,)), dma, dma((groups,)), dma, dma((groups,)),
                dma, dma((groups,)), dma, dma((8,)),
            ],
            compiler_params=pltpu.CompilerParams(collective_id=0, has_side_effects=True,
                                                 vmem_limit_bytes=VMEM_A),
        )(positions, tokens, w_query.reshape(8, cut, width), w_key.reshape(8, cut, hd), w_value.reshape(8, cut, hd),
          w_out, k_cache, v_cache)
        kept = pltpu.with_memory_space_constraint(kept, pltpu.VMEM)
        k_upd, v_upd, y, _ = pl.pallas_call(
            functools.partial(write_kernel, (n_seq, seq_local, n_blocks, slots)),
            out_shape=(jax.ShapeDtypeStruct(k_cache.shape, BF16),) * 2 + (jax.ShapeDtypeStruct(y.shape, BF16), held),
            in_specs=[smem, hbm, hbm, hbm, vmem, hbm, hbm],
            out_specs=(hbm, hbm, hbm, vmem),
            input_output_aliases={4: 3},
            scratch_shapes=[
                pltpu.VMEM((n_seq, hd), F32), pltpu.VMEM((n_seq, hd), F32), pltpu.VMEM(y.shape, BF16),
                pltpu.VMEM((RING, nh // 2, seq_local, hd), BF16), pltpu.VMEM((RING, nh // 2, seq_local, hd), BF16),
                dma((2, RING)), dma((2, RING)), dma((2, slots)), dma((3,)),
            ],
            compiler_params=pltpu.CompilerParams(vmem_limit_bytes=VMEM_B),
        )(positions, k_new, v_new, y, kept, k_cache, v_cache)
        return y.reshape(n_seq, width), k_upd, v_upd

    cache_spec = P('dp', 'sp', None)
    return jax.shard_map(local_step, mesh=mesh, in_specs=(P('dp', None), P(), P(), P(), P('sp', None), cache_spec, cache_spec, P('dp')), out_specs=(P('dp', None), cache_spec, cache_spec), check_vma=False)


VMEM_A = int(11.6 * 2**20)
VMEM_B = 10 << 20
```
